1024 devices in a mesh: seq: 16 (over x, y_hi, core), chan: 64 (over y_lo, z).
Axes of the slice: x: 4, y: 8 (y_hi: 2, y_lo: 4; y = y_hi * 4 + y_lo), z: 16, core: 2. Of those that a mesh axis runs over, the one named last changes fastest.
Arguments:
- features: bfloat16 [3, 4096, 2048], P(None, 'chan', 'seq'), may hold values from -6 to 6
- cotangent: bfloat16 [4096, 2048], P('chan', 'seq'), may hold values from -6 to 6
- long_filter: bfloat16 [4096, 2048], P('chan', 'seq'), may hold values from -0.125 to 0.125
- short_filters: float32 [3, 4096, 3], P(None, 'chan'), may hold values from -3.5 to 3.5
- skip_gain: float32 [4096], P('chan'), may hold values from -4 to 4
Outputs:
- gated_out: bfloat16 [4096, 2048], P('chan', 'seq')
- feature_grad: bfloat16 [3, 4096, 2048], P(None, 'chan', 'seq')
- long_grad: bfloat16 [4096, 2048], P('chan', 'seq')
- short_grad: float32 [3, 4096, 3], P(None, 'chan')
- skip_grad: float32 [4096], P('chan')
The draws below stay inside these ranges and needn't reach their ends.
All inputs are finite; a program needn't handle non-finite values.
Results may differ from the reference program's by a relative error of at most 0.015.
Values may be sent and summed in bfloat16 or wider, within the bound.
No kernel may reach another device: no remote copies, remote signals or barrier semaphores. Data moves between devices by JAX's collectives and lax.ppermute only.
A program may use at most 32 MiB of HBM per device.

```python
import math
import jax
import jax.numpy as jnp
from jax import lax

D = 4096
TAPS = 3
LEN = 2048


def block_levels(stream_key, extent, pieces, least, largest):
    factor_of = 1.0
    for position, parts in pieces:
        heights = jax.random.uniform(jax.random.fold_in(jax.random.fold_in(stream_key, 6), position), (parts,), jnp.float32, least / len(pieces), largest / len(pieces))
        factor_of = factor_of * jnp.repeat(jnp.exp(heights), extent[position] // parts).reshape((-1,) + (1,) * (len(extent) - 1 - position))
    return factor_of


def gaussian(stream_key, extent, spread, bound, pieces=(), kind=jnp.bfloat16):
    drawn = spread * jax.random.normal(stream_key, extent, jnp.float32)
    if pieces:
        drawn = drawn * block_levels(stream_key, extent, pieces, -0.22, 0.18)
    return jnp.clip(drawn, -bound, bound).astype(kind)


def setup_inputs(seed: int = 0) -> dict:
    keys = jax.random.split(jax.random.key(seed), 6)
    features = gaussian(keys[0], (3, D, LEN), 1.0, 6.0, ((1, 64), (2, 16)))
    cotangent = gaussian(keys[1], (D, LEN), 1.0, 6.0, ((0, 64), (1, 16)))
    long_filter = gaussian(keys[2], (D, LEN), LEN ** -0.5, 0.125, ((0, 64), (1, 16)))
    short_filters = gaussian(keys[3], (3, D, TAPS), TAPS ** -0.5, 3.5, ((1, 64),), jnp.float32)
    skip_gain = gaussian(keys[4], (D,), 1.0, 4.0, ((0, 64),), jnp.float32)
    return dict(features=features, cotangent=cotangent, long_filter=long_filter, short_filters=short_filters, skip_gain=skip_gain)


def delayed(values, offset):
    if offset == 0:
        return values
    padding = jnp.zeros(values.shape[:-1] + (offset,), values.dtype)
    return jnp.concatenate([padding, values[..., :-offset]], axis=-1)


def advanced(values, offset):
    if offset == 0:
        return values
    padding = jnp.zeros(values.shape[:-1] + (offset,), values.dtype)
    return jnp.concatenate([values[..., offset:], padding], axis=-1)


def long_terms(block):
    mixed_block, gated_block, kernel_block = block
    length = mixed_block.shape[-1]
    mixed_freq = jnp.fft.rfft(mixed_block, n=2 * length, axis=-1)
    gated_freq = jnp.fft.rfft(gated_block, n=2 * length, axis=-1)
    kernel_freq = jnp.fft.rfft(kernel_block, n=2 * length, axis=-1)
    conv_part = jnp.fft.irfft(mixed_freq * kernel_freq, n=2 * length, axis=-1)[:, :length]
    corr_part = jnp.fft.irfft(gated_freq * jnp.conj(kernel_freq), n=2 * length, axis=-1)[:, :length]
    cross_part = jnp.fft.irfft(gated_freq * jnp.conj(mixed_freq), n=2 * length, axis=-1)[:, :length]
    return conv_part.astype(jnp.float32), corr_part.astype(jnp.float32), cross_part.astype(jnp.float32)


def reference(features, cotangent, long_filter, short_filters, skip_gain):
    wide = features.astype(jnp.float32)
    primed = short_filters[:, :, 0:1] * wide
    for offset in range(1, TAPS):
        primed = primed + short_filters[:, :, offset:offset + 1] * delayed(wide, offset)
    mixed_term = (primed[1] * primed[2]).astype(jnp.bfloat16)
    cot_wide = cotangent.astype(jnp.float32)
    gated_grad = (cot_wide * primed[0]).astype(jnp.bfloat16)
    mixed_wide = mixed_term.astype(jnp.float32)
    gated_wide = gated_grad.astype(jnp.float32)
    block_rows = math.gcd(D, 256)
    block_count = D // block_rows
    blocks = (mixed_wide.reshape(block_count, block_rows, LEN),
              gated_wide.reshape(block_count, block_rows, LEN),
              long_filter.astype(jnp.float32).reshape(block_count, block_rows, LEN))
    conv_part, corr_part, cross_part = lax.map(long_terms, blocks)
    conv_part = conv_part.reshape(D, LEN)
    corr_part = corr_part.reshape(D, LEN)
    cross_part = cross_part.reshape(D, LEN)
    gain_column = skip_gain[:, None]
    long_out = (conv_part + gain_column * mixed_wide).astype(jnp.bfloat16)
    mixed_grad = (corr_part + gain_column * gated_wide).astype(jnp.bfloat16)
    long_wide = long_out.astype(jnp.float32)
    gated_out = (primed[0] * long_wide).astype(jnp.bfloat16)
    mixed_back = mixed_grad.astype(jnp.float32)
    primed_grad = jnp.stack([cot_wide * long_wide, mixed_back * primed[2], mixed_back * primed[1]])
    feature_grad = short_filters[:, :, 0:1] * primed_grad
    for offset in range(1, TAPS):
        feature_grad = feature_grad + short_filters[:, :, offset:offset + 1] * advanced(primed_grad, offset)
    short_grad = jnp.stack([jnp.sum(primed_grad * delayed(wide, offset), axis=-1) for offset in range(TAPS)], axis=-1)
    skip_grad = jnp.sum(gated_wide * mixed_wide, axis=-1)
    return gated_out, feature_grad.astype(jnp.bfloat16), cross_part.astype(jnp.bfloat16), short_grad, skip_grad
```

```python
import jax
import jax.numpy as jnp
from jax import lax
from jax.experimental import pallas as pl
from jax.experimental.pallas import tpu as pltpu
from jax.sharding import PartitionSpec as P

LANES = 128
ROWS = 24
STREAMS = 5
PIECES = 3

F32 = jnp.float32
BF16 = jnp.bfloat16


def iota(shape, dim):
    return lax.broadcasted_iota(jnp.int32, shape, dim)


def pack_kernel(features, cotangent, long_filter, out, wide, packed, *, groups, per_group):
    channels = groups * per_group
    for i in range(3):
        wide[i * channels : (i + 1) * channels, :] = features[i].astype(F32)
    wide[3 * channels : 4 * channels, :] = cotangent[...].astype(F32)
    wide[4 * channels : 5 * channels, :] = long_filter[...].astype(F32)
    for i in range(STREAMS):
        for c in range(per_group):
            rows = wide[pl.ds(i * channels + c, groups, stride=per_group), :]
            packed[pl.ds(i * per_group + c, groups, stride=ROWS), :] = rows
    for r in range(STREAMS * per_group, ROWS):
        packed[pl.ds(r, groups, stride=ROWS), :] = jnp.zeros((groups, LANES), F32)
    out[...] = packed[...].reshape(groups, ROWS, LANES).astype(BF16)


def shifted_down(values, count):
    if count == 0:
        return values
    size = values.shape[0]
    return jnp.where(iota(values.shape, 0) >= count, pltpu.roll(values, count, 0), 0.0)


def shifted_up(values, count):
    if count == 0:
        return values
    size = values.shape[0]
    return jnp.where(iota(values.shape, 0) < size - count, pltpu.roll(values, size - count, 0), 0.0)


def delayed(values, offset):
    if offset == 0:
        return values
    turned = pltpu.roll(values, offset, 1)
    return jnp.where(iota(values.shape, 1) >= offset, turned, shifted_down(turned, 1))


def advanced(values, offset):
    if offset == 0:
        return values
    turned = pltpu.roll(values, LANES - offset, 1)
    return jnp.where(iota(values.shape, 1) < LANES - offset, turned, shifted_up(turned, 1))


def fill_toeplitz(rows, target):
    square = (LANES, LANES)
    keep = iota(square, 1) >= iota(square, 0)
    before = jnp.zeros(square, F32)
    for k in range(rows.shape[0]):
        line = jnp.broadcast_to(rows[k : k + 1, :], square)
        turned = pltpu.roll(line, 0, 1, stride=1, stride_axis=0)
        target[:, k * LANES : (k + 1) * LANES] = jnp.where(keep, turned, before).astype(BF16)
        before = turned


def middle_kernel(where, weights, gain, received, out, wide, packed, filter_band, mixed_band):
    blocks = received.shape[0]
    per_group = weights.shape[2] // blocks
    taps = weights.shape[1]
    wide[...] = received[...].astype(F32).reshape(blocks * ROWS, LANES)
    first = where[0] * per_group
    sums = []
    for c in range(per_group):

        def stream(i):
            return wide[pl.ds(i * per_group + c, blocks, stride=ROWS), :]

        def put(i, values):
            packed[pl.ds(i * per_group + c, blocks, stride=ROWS), :] = values

        w = [[weights[i, o, first + c] for o in range(taps)] for i in range(3)]
        local_gain = gain[first + c]
        history = [[delayed(stream(i), o) for o in range(taps)] for i in range(3)]
        primed = []
        for i in range(3):
            running = w[i][0] * history[i][0]
            for o in range(1, taps):
                running = running + w[i][o] * history[i][o]
            primed.append(running)
        cot = stream(3)
        mixed = (primed[1] * primed[2]).astype(BF16).astype(F32)
        gated = (cot * primed[0]).astype(BF16).astype(F32)
        fill_toeplitz(stream(4), filter_band)
        fill_toeplitz(mixed, mixed_band)
        spread = jnp.dot(mixed.astype(BF16), filter_band[...], preferred_element_type=F32)
        conv = spread[:, 0:LANES]
        for k in range(1, blocks):
            conv = conv + shifted_down(spread[:, k * LANES : (k + 1) * LANES], k)
        ahead = jnp.concatenate([shifted_up(gated, k).astype(BF16) for k in range(blocks)], axis=1)
        across = (((1,), (1,)), ((), ()))
        corr = lax.dot_general(ahead, filter_band[...], across, preferred_element_type=F32)
        cross = lax.dot_general(ahead, mixed_band[...], across, preferred_element_type=F32)
        long_out = (conv + local_gain * mixed).astype(BF16).astype(F32)
        mixed_grad = (corr + local_gain * gated).astype(BF16).astype(F32)
        primed_grad = [cot * long_out, mixed_grad * primed[2], mixed_grad * primed[1]]
        put(0, primed[0] * long_out)
        for i in range(3):
            running = w[i][0] * primed_grad[i]
            for o in range(1, taps):
                running = running + w[i][o] * advanced(primed_grad[i], o)
            put(1 + i, running)
        put(4, cross)
        for i in range(3):
            for o in range(taps):
                sums.append(jnp.sum(primed_grad[i] * history[i][o], axis=0, keepdims=True))
        sums.append(jnp.sum(gated * mixed, axis=0, keepdims=True))
    count = len(sums)
    totals = jnp.sum(jnp.concatenate(sums, axis=0), axis=1, keepdims=True)
    shape = (count, LANES)
    line = jnp.sum(jnp.where(iota(shape, 0) == iota(shape, 1), totals, 0.0), axis=0, keepdims=True)
    line = jnp.broadcast_to(line, (8, LANES))
    left, row = line, jnp.zeros_like(line)
    for p in range(PIECES):
        piece = left.astype(BF16).astype(F32)
        left = left - piece
        row = row + (pltpu.roll(piece, p * count, 1) if p else piece)
    row = jnp.broadcast_to(row[0:1, :], (blocks, LANES))
    used = STREAMS * per_group
    packed[pl.ds(used, blocks, stride=ROWS), :] = row
    for r in range(used + 1, ROWS):
        packed[pl.ds(r, blocks, stride=ROWS), :] = jnp.zeros((blocks, LANES), F32)
    out[...] = packed[...].reshape(blocks, ROWS, LANES).astype(BF16)


def unpack_kernel(
    received, gated_out, feature_grad, long_grad, short_grad, skip_grad, wide, rows_out, *, per_group
):
    groups = received.shape[0]
    channels = groups * per_group
    wide[...] = received[...].astype(F32).reshape(groups * ROWS, LANES)
    for i in range(STREAMS):
        for c in range(per_group):
            rows = wide[pl.ds(i * per_group + c, groups, stride=ROWS), :]
            rows_out[pl.ds(i * channels + c, groups, stride=per_group), :] = rows
    gated_out[...] = rows_out[0:channels, :].astype(BF16)
    for i in range(3):
        feature_grad[i] = rows_out[(1 + i) * channels : (2 + i) * channels, :].astype(BF16)
    long_grad[...] = rows_out[4 * channels : 5 * channels, :].astype(BF16)
    pieces = wide[pl.ds(STREAMS * per_group, groups, stride=ROWS), :].astype(BF16)
    taps = short_grad.shape[1]
    each = 3 * taps + 1
    shape = (groups, LANES)
    owner = (iota(shape, 1) // per_group == iota(shape, 0)).astype(F32).astype(BF16)
    turned = lax.dot_general(pieces, owner, (((0,), (0,)), ((), ())), preferred_element_type=F32)
    place = iota((each, LANES), 1) % per_group
    total = jnp.zeros((each, LANES), F32)
    for c in range(per_group):
        value = jnp.zeros((each, LANES), F32)
        for p in range(PIECES):
            at = (p * per_group + c) * each
            value = value + turned[at : at + each, :]
        total = jnp.where(place == c, value, total)
    for i in range(3):
        short_grad[i] = total[i * taps : (i + 1) * taps, 0:channels]
    skip_grad[...] = total[3 * taps : 3 * taps + 1, 0:channels]


def vmem(shape, dtype=F32):
    return pltpu.VMEM(shape, dtype)


def solution(mesh):
    groups = mesh.shape["seq"]

    def exchange(parts):
        return lax.all_to_all(parts, "seq", split_axis=0, concat_axis=0, tiled=True)

    def shards(features, cotangent, long_filter, short_filters, skip_gain):
        channels = features.shape[1]
        per_group = channels // groups
        taps = short_filters.shape[2]
        whole = pl.BlockSpec(memory_space=pltpu.VMEM)
        scalars = pl.BlockSpec(memory_space=pltpu.SMEM)
        parts_shape = jax.ShapeDtypeStruct((groups, ROWS, LANES), BF16)
        flat = (groups * ROWS, LANES)
        tall = (STREAMS * channels, LANES)
        parts = pl.pallas_call(
            lambda *refs: pack_kernel(*refs, groups=groups, per_group=per_group),
            name="pack",
            out_shape=parts_shape,
            in_specs=[whole] * 3,
            out_specs=whole,
            scratch_shapes=[vmem(tall), vmem(flat)],
        )(features, cotangent, long_filter)
        columns = exchange(parts)
        where = lax.axis_index("seq").astype(jnp.int32).reshape(1)
        band = (LANES, groups * LANES)
        results = pl.pallas_call(
            middle_kernel,
            name="middle",
            out_shape=parts_shape,
            in_specs=[scalars, scalars, scalars, whole],
            out_specs=whole,
            scratch_shapes=[vmem(flat), vmem(flat), vmem(band, BF16), vmem(band, BF16)],
        )(where, jnp.swapaxes(short_filters, 1, 2), skip_gain, columns)
        back = exchange(results)
        gated_out, feature_grad, long_grad, short_grad, skip_grad = pl.pallas_call(
            lambda *refs: unpack_kernel(*refs, per_group=per_group),
            name="unpack",
            out_shape=(
                jax.ShapeDtypeStruct((channels, LANES), BF16),
                jax.ShapeDtypeStruct((3, channels, LANES), BF16),
                jax.ShapeDtypeStruct((channels, LANES), BF16),
                jax.ShapeDtypeStruct((3, taps, channels), F32),
                jax.ShapeDtypeStruct((1, channels), F32),
            ),
            in_specs=[whole],
            out_specs=(whole,) * 5,
            scratch_shapes=[vmem(flat), vmem(tall)],
        )(back)
        return (
            gated_out,
            feature_grad,
            long_grad,
            jnp.swapaxes(short_grad, 1, 2),
            skip_grad.reshape(channels),
        )

    return jax.shard_map(
        shards,
        mesh=mesh,
        in_specs=(
            P(None, "chan", "seq"),
            P("chan", "seq"),
            P("chan", "seq"),
            P(None, "chan", None),
            P("chan"),
        ),
        out_specs=(
            P("chan", "seq"),
            P(None, "chan", "seq"),
            P("chan", "seq"),
            P(None, "chan", None),
            P("chan"),
        ),
        check_vma=False,
    )
```

```python
import jax
import jax.numpy as jnp
from jax import lax
from jax.experimental import pallas as pl
from jax.experimental.pallas import tpu as pltpu
from jax.sharding import PartitionSpec as P

LANES = 128
ROWS = 24
STREAMS = 5
PIECES = 3

F32 = jnp.float32
BF16 = jnp.bfloat16


def iota(shape, dim):
    return lax.broadcasted_iota(jnp.int32, shape, dim)


def pack_kernel(features, cotangent, long_filter, out, wide, packed, *, groups, per_group):
    channels = groups * per_group
    for i in range(3):
        wide[i * channels : (i + 1) * channels, :] = features[i].astype(F32)
    wide[3 * channels : 4 * channels, :] = cotangent[...].astype(F32)
    wide[4 * channels : 5 * channels, :] = long_filter[...].astype(F32)
    for i in range(STREAMS):
        for c in range(per_group):
            rows = wide[pl.ds(i * channels + c, groups, stride=per_group), :]
            packed[pl.ds(i * per_group + c, groups, stride=ROWS), :] = rows
    for r in range(STREAMS * per_group, ROWS):
        packed[pl.ds(r, groups, stride=ROWS), :] = jnp.zeros((groups, LANES), F32)
    out[...] = packed[...].reshape(groups, ROWS, LANES).astype(BF16)


def shifted_down(values, count):
    if count == 0:
        return values
    size = values.shape[0]
    return jnp.where(iota(values.shape, 0) >= count, pltpu.roll(values, count, 0), 0.0)


def shifted_up(values, count):
    if count == 0:
        return values
    size = values.shape[0]
    return jnp.where(iota(values.shape, 0) < size - count, pltpu.roll(values, size - count, 0), 0.0)


def delayed(values, offset):
    if offset == 0:
        return values
    turned = pltpu.roll(values, offset, 1)
    return jnp.where(iota(values.shape, 1) >= offset, turned, shifted_down(turned, 1))


def advanced(values, offset):
    if offset == 0:
        return values
    turned = pltpu.roll(values, LANES - offset, 1)
    return jnp.where(iota(values.shape, 1) < LANES - offset, turned, shifted_up(turned, 1))


def fill_toeplitz(rows, target):
    square = (LANES, LANES)
    keep = iota(square, 1) >= iota(square, 0)
    before = jnp.zeros(square, F32)
    for k in range(rows.shape[0]):
        line = jnp.broadcast_to(rows[k : k + 1, :], square)
        turned = pltpu.roll(line, 0, 1, stride=1, stride_axis=0)
        target[:, k * LANES : (k + 1) * LANES] = jnp.where(keep, turned, before).astype(BF16)
        before = turned


def middle_kernel(weights, gain, received, out, wide, packed, filter_band, mixed_band):
    blocks = received.shape[0]
    per_group = weights.shape[2] // blocks
    taps = weights.shape[1]
    wide[...] = received[...].astype(F32).reshape(blocks * ROWS, LANES)
    first = lax.axis_index("seq") * per_group
    sums = []
    for c in range(per_group):

        def stream(i):
            return wide[pl.ds(i * per_group + c, blocks, stride=ROWS), :]

        def put(i, values):
            packed[pl.ds(i * per_group + c, blocks, stride=ROWS), :] = values

        w = [[weights[i, o, first + c] for o in range(taps)] for i in range(3)]
        local_gain = gain[first + c]
        history = [[delayed(stream(i), o) for o in range(taps)] for i in range(3)]
        primed = []
        for i in range(3):
            running = w[i][0] * history[i][0]
            for o in range(1, taps):
                running = running + w[i][o] * history[i][o]
            primed.append(running)
        cot = stream(3)
        mixed = (primed[1] * primed[2]).astype(BF16).astype(F32)
        gated = (cot * primed[0]).astype(BF16).astype(F32)
        fill_toeplitz(stream(4), filter_band)
        fill_toeplitz(mixed, mixed_band)
        spread = jnp.dot(mixed.astype(BF16), filter_band[...], preferred_element_type=F32)
        conv = spread[:, 0:LANES]
        for k in range(1, blocks):
            conv = conv + shifted_down(spread[:, k * LANES : (k + 1) * LANES], k)
        ahead = jnp.concatenate([shifted_up(gated, k).astype(BF16) for k in range(blocks)], axis=1)
        across = (((1,), (1,)), ((), ()))
        corr = lax.dot_general(ahead, filter_band[...], across, preferred_element_type=F32)
        cross = lax.dot_general(ahead, mixed_band[...], across, preferred_element_type=F32)
        long_out = (conv + local_gain * mixed).astype(BF16).astype(F32)
        mixed_grad = (corr + local_gain * gated).astype(BF16).astype(F32)
        primed_grad = [cot * long_out, mixed_grad * primed[2], mixed_grad * primed[1]]
        put(0, primed[0] * long_out)
        for i in range(3):
            running = w[i][0] * primed_grad[i]
            for o in range(1, taps):
                running = running + w[i][o] * advanced(primed_grad[i], o)
            put(1 + i, running)
        put(4, cross)
        for i in range(3):
            for o in range(taps):
                sums.append(jnp.sum(primed_grad[i] * history[i][o], axis=0, keepdims=True))
        sums.append(jnp.sum(gated * mixed, axis=0, keepdims=True))
    count = len(sums)
    totals = jnp.sum(jnp.concatenate(sums, axis=0), axis=1, keepdims=True)
    shape = (count, LANES)
    line = jnp.sum(jnp.where(iota(shape, 0) == iota(shape, 1), totals, 0.0), axis=0, keepdims=True)
    line = jnp.broadcast_to(line, (8, LANES))
    left, row = line, jnp.zeros_like(line)
    for p in range(PIECES):
        piece = left.astype(BF16).astype(F32)
        left = left - piece
        row = row + (pltpu.roll(piece, p * count, 1) if p else piece)
    row = jnp.broadcast_to(row[0:1, :], (blocks, LANES))
    used = STREAMS * per_group
    packed[pl.ds(used, blocks, stride=ROWS), :] = row
    for r in range(used + 1, ROWS):
        packed[pl.ds(r, blocks, stride=ROWS), :] = jnp.zeros((blocks, LANES), F32)
    out[...] = packed[...].reshape(blocks, ROWS, LANES).astype(BF16)


def unpack_kernel(
    received, gated_out, feature_grad, long_grad, short_grad, skip_grad, wide, rows_out, *, per_group
):
    groups = received.shape[0]
    channels = groups * per_group
    wide[...] = received[...].astype(F32).reshape(groups * ROWS, LANES)
    for i in range(STREAMS):
        for c in range(per_group):
            rows = wide[pl.ds(i * per_group + c, groups, stride=ROWS), :]
            rows_out[pl.ds(i * channels + c, groups, stride=per_group), :] = rows
    gated_out[...] = rows_out[0:channels, :].astype(BF16)
    for i in range(3):
        feature_grad[i] = rows_out[(1 + i) * channels : (2 + i) * channels, :].astype(BF16)
    long_grad[...] = rows_out[4 * channels : 5 * channels, :].astype(BF16)
    pieces = wide[pl.ds(STREAMS * per_group, groups, stride=ROWS), :].astype(BF16)
    taps = short_grad.shape[1]
    each = 3 * taps + 1
    shape = (groups, LANES)
    owner = (iota(shape, 1) // per_group == iota(shape, 0)).astype(F32).astype(BF16)
    turned = lax.dot_general(pieces, owner, (((0,), (0,)), ((), ())), preferred_element_type=F32)
    place = iota((each, LANES), 1) % per_group
    total = jnp.zeros((each, LANES), F32)
    for c in range(per_group):
        value = jnp.zeros((each, LANES), F32)
        for p in range(PIECES):
            at = (p * per_group + c) * each
            value = value + turned[at : at + each, :]
        total = jnp.where(place == c, value, total)
    for i in range(3):
        short_grad[i] = total[i * taps : (i + 1) * taps, 0:channels]
    skip_grad[...] = total[3 * taps : 3 * taps + 1, 0:channels]


def vmem(shape, dtype=F32):
    return pltpu.VMEM(shape, dtype)


def solution(mesh):
    groups = mesh.shape["seq"]

    def exchange(parts):
        return lax.all_to_all(parts, "seq", split_axis=0, concat_axis=0, tiled=True)

    def shards(features, cotangent, long_filter, short_filters, skip_gain):
        channels = features.shape[1]
        per_group = channels // groups
        taps = short_filters.shape[2]
        whole = pl.BlockSpec(memory_space=pltpu.VMEM)
        scalars = pl.BlockSpec(memory_space=pltpu.SMEM)
        parts_shape = jax.ShapeDtypeStruct((groups, ROWS, LANES), BF16)
        flat = (groups * ROWS, LANES)
        tall = (STREAMS * channels, LANES)
        parts = pl.pallas_call(
            lambda *refs: pack_kernel(*refs, groups=groups, per_group=per_group),
            name="pack",
            compiler_params=pltpu.CompilerParams(vmem_limit_bytes=4 << 20),
            out_shape=parts_shape,
            in_specs=[whole] * 3,
            out_specs=whole,
            scratch_shapes=[vmem(tall), vmem(flat)],
        )(features, cotangent, long_filter)
        columns = exchange(parts)
        band = (LANES, groups * LANES)
        results = pl.pallas_call(
            middle_kernel,
            name="middle",
            compiler_params=pltpu.CompilerParams(vmem_limit_bytes=8 << 20),
            out_shape=parts_shape,
            in_specs=[scalars, scalars, whole],
            out_specs=whole,
            scratch_shapes=[vmem(flat), vmem(flat), vmem(band, BF16), vmem(band, BF16)],
        )(jnp.swapaxes(short_filters, 1, 2), skip_gain, columns)
        back = exchange(results)
        gated_out, feature_grad, long_grad, short_grad, skip_grad = pl.pallas_call(
            lambda *refs: unpack_kernel(*refs, per_group=per_group),
            name="unpack",
            compiler_params=pltpu.CompilerParams(vmem_limit_bytes=4 << 20),
            out_shape=(
                jax.ShapeDtypeStruct((channels, LANES), BF16),
                jax.ShapeDtypeStruct((3, channels, LANES), BF16),
                jax.ShapeDtypeStruct((channels, LANES), BF16),
                jax.ShapeDtypeStruct((3, taps, channels), F32),
                jax.ShapeDtypeStruct((1, channels), F32),
            ),
            in_specs=[whole],
            out_specs=(whole,) * 5,
            scratch_shapes=[vmem(flat), vmem(tall)],
        )(back)
        return (
            gated_out,
            feature_grad,
            long_grad,
            jnp.swapaxes(short_grad, 1, 2),
            skip_grad.reshape(channels),
        )

    return jax.shard_map(
        shards,
        mesh=mesh,
        in_specs=(
            P(None, "chan", "seq"),
            P("chan", "seq"),
            P("chan", "seq"),
            P(None, "chan", None),
            P("chan"),
        ),
        out_specs=(
            P("chan", "seq"),
            P(None, "chan", "seq"),
            P("chan", "seq"),
            P(None, "chan", None),
            P("chan"),
        ),
        check_vma=False,
    )
```

```python
import jax
import jax.numpy as jnp
from jax import lax
from jax.experimental import pallas as pl
from jax.experimental.pallas import tpu as pltpu
from jax.sharding import Mesh
from jax.sharding import PartitionSpec as P

SEQ = ("x", "y", "c")
SIDES = (4, 2, 2)
OWNERS = ("x", "c")
BLOCKS = 16
GROUPS = 8
EACH = 8
LANES = 128
STREAMS = 5
TAPS = 3
SUMS = 3 * TAPS + 1
PIECES = 3
IN_ROWS = STREAMS * EACH
OUT_ROWS = IN_ROWS + 8
PHASES = 4
STEP = LANES // PHASES

F32 = jnp.float32
BF16 = jnp.bfloat16


def iota(shape, dim):
    return lax.broadcasted_iota(jnp.int32, shape, dim)


def pack_kernel(features, cotangent, long_filter, weights, gain, out, table, taps, gains, sems):
    small = [
        pltpu.make_async_copy(weights, taps, sems.at[0]),
        pltpu.make_async_copy(gain, gains, sems.at[1]),
    ]
    sources = [features.at[i] for i in range(3)] + [cotangent, long_filter]
    large = []
    for i, source in enumerate(sources):
        for y in range(SIDES[1]):
            target = out.at[:, y, :, pl.ds(i * EACH, EACH), :]
            large.append(pltpu.make_async_copy(source, target, sems.at[2 + 2 * i + y]))
    for copy in small + large:
        copy.start()
    for copy in small:
        copy.wait()
    first = (lax.axis_index("x") * SIDES[2] + lax.axis_index("c")) * EACH
    channels = gains.shape[1]
    shape = (EACH, channels)
    chosen = iota(shape, 1) == iota(shape, 0) + first
    for j in range(SUMS):
        line = gains[...] if j == 3 * TAPS else taps[j // TAPS, j % TAPS : j % TAPS + 1, :]
        line = jnp.broadcast_to(line, shape)
        column = jnp.sum(jnp.where(chosen, line, 0.0), axis=1, keepdims=True)
        table[j] = jnp.broadcast_to(column, (EACH, LANES))
    for copy in large:
        copy.wait()


def shifted_down(values, count):
    if count == 0:
        return values
    return jnp.where(iota(values.shape, 0) >= count, pltpu.roll(values, count, 0), 0.0)


def shifted_up(values, count):
    if count == 0:
        return values
    size = values.shape[0]
    return jnp.where(iota(values.shape, 0) < size - count, pltpu.roll(values, size - count, 0), 0.0)


def later(values, count, carry):
    if count == 0:
        return values
    turned = pltpu.roll(values, count, 1)
    return jnp.where(iota(values.shape, 1) >= count, turned, carry(turned, 1))


def earlier(values, count):
    if count == 0:
        return values
    turned = pltpu.roll(values, LANES - count, 1)
    return jnp.where(iota(values.shape, 1) < LANES - count, turned, shifted_up(turned, 1))


def fill_right(line_of, right, column):
    shape = (STEP, LANES)
    keep = iota(shape, 1) >= iota(shape, 0)
    before = jnp.zeros(shape, F32)
    for k in range(BLOCKS):
        line = jnp.broadcast_to(line_of(k), shape)
        turned = pltpu.roll(line, 0, 1, stride=1, stride_axis=0)
        part = jnp.where(keep, turned, before).astype(BF16)
        right[k * STEP : (k + 1) * STEP, column : column + LANES] = part
        before = turned


def left_rows(values, shifted):
    turned = [pltpu.roll(values, STEP * q, 1) if q else values for q in range(PHASES)]
    moved = [[shifted(turned[q], kk) for q in range(PHASES)] for kk in range(PHASES)]
    part = iota(values.shape, 1) // STEP
    rows = []
    for p in range(PHASES):
        base = moved[0][-p % PHASES]
        for kk in range(1, PHASES):
            base = jnp.where(part == kk, moved[kk][(kk - p) % PHASES], base)
        tiles = [shifted(base, PHASES * j).astype(BF16) for j in range(BLOCKS // PHASES)]
        rows.append(jnp.concatenate(tiles, axis=1))
    return rows


def joined(parts, carry):
    total = parts[0]
    for p in range(1, PHASES):
        total = total + later(parts[p], STEP * p, carry)
    return total


def middle_kernel(table, received, out, wide, packed, right, kept, mirrored, turned_back):
    wide[...] = received[...].astype(F32).reshape(BLOCKS * IN_ROWS, LANES)
    square = (LANES, LANES)
    mirror = jnp.where(iota(square, 0) + iota(square, 1) == LANES - 1, 1.0, 0.0).astype(BF16)

    def stream(i, c):
        return wide[pl.ds(i * EACH + c, BLOCKS, stride=IN_ROWS), :]

    def put(i, c, values):
        packed[pl.ds(i * EACH + c, BLOCKS, stride=OUT_ROWS), :] = values

    def weight(j, c):
        return table[j, c : c + 1, :]

    def rows(c):
        return slice(c * BLOCKS, (c + 1) * BLOCKS)

    PRIMED, MIXED, GATED, HISTORY, LONG = 0, 3, 4, 5, 11
    for c in range(EACH):
        primed = []
        for i in range(3):
            value = stream(i, c)
            running = weight(i * TAPS, c) * value
            for o in range(1, TAPS):
                moved = later(value, o, shifted_down)
                kept[HISTORY + 2 * i + o - 1, rows(c), :] = moved
                running = running + weight(i * TAPS + o, c) * moved
            kept[PRIMED + i, rows(c), :] = running
            primed.append(running)
        kept[MIXED, rows(c), :] = (primed[1] * primed[2]).astype(BF16).astype(F32)
        kept[GATED, rows(c), :] = (stream(3, c) * primed[0]).astype(BF16).astype(F32)
    mirrored[...] = jnp.dot(kept[GATED].astype(BF16), mirror, preferred_element_type=F32)
    half = EACH * BLOCKS
    for c in range(EACH):
        gain = weight(3 * TAPS, c)
        mixed = kept[MIXED, rows(c), :]
        gated = mirrored[rows(c), :]
        fill_right(lambda k: wide[k * IN_ROWS + 4 * EACH + c : k * IN_ROWS + 4 * EACH + c + 1, :], right.at[c], 0)
        fill_right(lambda k: kept[MIXED, c * BLOCKS + k : c * BLOCKS + k + 1, :], right.at[c], LANES)
        left = jnp.concatenate(left_rows(mixed, shifted_down) + left_rows(gated, shifted_up), axis=0)
        product = jnp.dot(left, right[c], preferred_element_type=F32)

        def parts(at, column):
            cut = slice(column, column + LANES)
            return [product[at + p * BLOCKS : at + (p + 1) * BLOCKS, cut] for p in range(PHASES)]

        conv = joined(parts(0, 0), shifted_down)
        corr = joined(parts(PHASES * BLOCKS, 0), shifted_up)
        cross = joined(parts(PHASES * BLOCKS, LANES), shifted_up)
        kept[LONG, rows(c), :] = (conv + gain * mixed).astype(BF16).astype(F32)
        turned_back[rows(c), :] = corr + gain * gated
        turned_back[half + c * BLOCKS : half + (c + 1) * BLOCKS, :] = cross
    turned_back[...] = jnp.dot(turned_back[...].astype(BF16), mirror, preferred_element_type=F32)
    sums = [[] for _ in range(SUMS)]
    for c in range(EACH):
        cot = stream(3, c)
        primed = [kept[PRIMED + i, rows(c), :] for i in range(3)]
        long_out = kept[LONG, rows(c), :]
        mixed_grad = turned_back[rows(c), :]
        primed_grad = [cot * long_out, mixed_grad * primed[2], mixed_grad * primed[1]]
        put(0, c, primed[0] * long_out)
        put(4, c, turned_back[half + c * BLOCKS : half + (c + 1) * BLOCKS, :])
        for i in range(3):
            running = weight(i * TAPS, c) * primed_grad[i]
            for o in range(1, TAPS):
                running = running + weight(i * TAPS + o, c) * earlier(primed_grad[i], o)
            put(1 + i, c, running)
            for o in range(TAPS):
                past = kept[HISTORY + 2 * i + o - 1, rows(c), :] if o else stream(i, c)
                sums[i * TAPS + o].append(jnp.sum(primed_grad[i] * past, axis=0, keepdims=True))
        both = kept[GATED, rows(c), :] * kept[MIXED, rows(c), :]
        sums[3 * TAPS].append(jnp.sum(both, axis=0, keepdims=True))
    stacked = jnp.concatenate([line for lines in sums for line in lines], axis=0)
    totals = jnp.sum(stacked, axis=1, keepdims=True)
    shape = stacked.shape
    line = jnp.sum(jnp.where(iota(shape, 0) == iota(shape, 1), totals, 0.0), axis=0, keepdims=True)
    left = jnp.broadcast_to(line, (BLOCKS, LANES))
    for r in range(IN_ROWS, OUT_ROWS):
        piece = left.astype(BF16).astype(F32)
        if r >= IN_ROWS + PIECES:
            piece = jnp.zeros_like(piece)
        left = left - piece
        packed[pl.ds(r, BLOCKS, stride=OUT_ROWS), :] = piece
    side = lax.axis_index("y")
    wanted = SIDES[2] * OUT_ROWS
    for x in range(SIDES[0]):
        at = pl.multiple_of((SIDES[1] * x + side) * wanted, 8)
        block = packed[pl.ds(at, wanted), :].astype(BF16)
        out[SIDES[2] * x : SIDES[2] * (x + 1)] = block.reshape(SIDES[2], OUT_ROWS, LANES)


def unpack_kernel(
    received, gated_out, feature_grad, long_grad, short_grad, skip_grad, taps, gains, sems
):
    targets = [gated_out] + [feature_grad.at[i] for i in range(3)] + [long_grad]
    copies = []
    for i, target in enumerate(targets):
        source = received.at[:, pl.ds(i * EACH, EACH), :]
        copies.append(pltpu.make_async_copy(source, target, sems.at[i]))
        copies[-1].start()
    pieces = received[:, IN_ROWS:OUT_ROWS, :].astype(F32)
    shape = (GROUPS, LANES)
    owner = jnp.where(iota(shape, 1) // EACH == iota(shape, 0), 1.0, 0.0).astype(BF16)
    total = jnp.zeros((LANES, LANES), F32)
    for p in range(PIECES):
        piece = pieces[:, p, :].astype(BF16)
        total = total + lax.dot_general(
            piece, owner, (((0,), (0,)), ((), ())), preferred_element_type=F32
        )
    total = total[: SUMS * EACH, :].reshape(SUMS, EACH, LANES)
    mine = iota(total.shape, 1) == iota(total.shape, 2) % EACH
    lines = jnp.sum(jnp.where(mine, total, 0.0), axis=1)
    channels = gains.shape[1]
    for i in range(3):
        taps[i] = lines[i * TAPS : (i + 1) * TAPS, 0:channels]
    gains[...] = lines[3 * TAPS :, 0:channels]
    last = [
        pltpu.make_async_copy(taps, short_grad, sems.at[STREAMS]),
        pltpu.make_async_copy(gains, skip_grad, sems.at[STREAMS + 1]),
    ]
    for copy in last:
        copy.start()
    for copy in copies + last:
        copy.wait()


def grant(mebibytes):
    return pltpu.CompilerParams(vmem_limit_bytes=mebibytes << 20)


def shards(features, cotangent, long_filter, short_filters, skip_gain):
    channels = features.shape[1]
    whole = pl.BlockSpec(memory_space=pltpu.VMEM)
    far = pl.BlockSpec(memory_space=pltpu.HBM)
    cut = (SIDES[0], SIDES[2], EACH, LANES)
    parts, table = pl.pallas_call(
        pack_kernel,
        name="pack",
        compiler_params=grant(4),
        out_shape=(
            jax.ShapeDtypeStruct((*SIDES, IN_ROWS, LANES), BF16),
            jax.ShapeDtypeStruct((SUMS, EACH, LANES), F32),
        ),
        in_specs=[far] * 5,
        out_specs=(whole, whole),
        scratch_shapes=[
            pltpu.VMEM((3, TAPS, channels), F32),
            pltpu.VMEM((1, channels), F32),
            pltpu.SemaphoreType.DMA((2 + 2 * STREAMS,)),
        ],
    )(
        features.reshape(3, *cut),
        cotangent.reshape(cut),
        long_filter.reshape(cut),
        jnp.swapaxes(short_filters, 1, 2),
        skip_gain.reshape(1, channels),
    )
    columns = lax.all_to_all(
        parts.reshape(BLOCKS, IN_ROWS, LANES), SEQ, split_axis=0, concat_axis=0, tiled=True
    )
    results = pl.pallas_call(
        middle_kernel,
        name="middle",
        compiler_params=grant(12),
        out_shape=jax.ShapeDtypeStruct((GROUPS, OUT_ROWS, LANES), BF16),
        in_specs=[whole, whole],
        out_specs=whole,
        scratch_shapes=[
            pltpu.VMEM((BLOCKS * IN_ROWS, LANES), F32),
            pltpu.VMEM((BLOCKS * OUT_ROWS, LANES), F32),
            pltpu.VMEM((EACH, BLOCKS * STEP, 2 * LANES), BF16),
            pltpu.VMEM((12, EACH * BLOCKS, LANES), F32),
            pltpu.VMEM((EACH * BLOCKS, LANES), F32),
            pltpu.VMEM((2 * EACH * BLOCKS, LANES), F32),
        ],
    )(table, columns)
    back = lax.all_to_all(results, OWNERS, split_axis=0, concat_axis=0, tiled=True)
    block = (GROUPS, EACH, LANES)
    gated_out, feature_grad, long_grad, short_grad, skip_grad = pl.pallas_call(
        unpack_kernel,
        name="unpack",
        compiler_params=grant(4),
        out_shape=(
            jax.ShapeDtypeStruct(block, BF16),
            jax.ShapeDtypeStruct((3, *block), BF16),
            jax.ShapeDtypeStruct(block, BF16),
            jax.ShapeDtypeStruct((3, TAPS, channels), F32),
            jax.ShapeDtypeStruct((1, channels), F32),
        ),
        in_specs=[whole],
        out_specs=(far,) * 5,
        scratch_shapes=[
            pltpu.VMEM((3, TAPS, channels), F32),
            pltpu.VMEM((1, channels), F32),
            pltpu.SemaphoreType.DMA((STREAMS + 2,)),
        ],
    )(back)
    return (
        gated_out.reshape(channels, LANES),
        feature_grad.reshape(3, channels, LANES),
        long_grad.reshape(channels, LANES),
        jnp.swapaxes(short_grad, 1, 2),
        skip_grad.reshape(channels),
    )


def solution(mesh):
    torus = Mesh(mesh.devices.reshape(*SIDES, mesh.shape["chan"]), (*SEQ, "chan"))
    return jax.shard_map(
        shards,
        mesh=torus,
        in_specs=(
            P(None, "chan", SEQ),
            P("chan", SEQ),
            P("chan", SEQ),
            P(None, "chan", None),
            P("chan"),
        ),
        out_specs=(
            P("chan", SEQ),
            P(None, "chan", SEQ),
            P("chan", SEQ),
            P(None, "chan", None),
            P("chan"),
        ),
        check_vma=False,
    )
```

```python
import jax
import jax.numpy as jnp
from jax import lax
from jax.experimental import pallas as pl
from jax.experimental.pallas import tpu as pltpu
from jax.sharding import Mesh
from jax.sharding import PartitionSpec as P

SEQ = ("x", "y", "c")
SIDES = (4, 2, 2)
OWNERS = ("x", "c")
BLOCKS = 16
GROUPS = 8
EACH = 8
LANES = 128
STREAMS = 5
TAPS = 3
SUMS = 3 * TAPS + 1
PIECES = 3
IN_ROWS = STREAMS * EACH
OUT_ROWS = IN_ROWS + 8
PHASES = 4
STEP = LANES // PHASES

F32 = jnp.float32
BF16 = jnp.bfloat16


def iota(shape, dim):
    return lax.broadcasted_iota(jnp.int32, shape, dim)


def pack_kernel(features, cotangent, long_filter, weights, gain, out, table, taps, gains, sems):
    small = [
        pltpu.make_async_copy(weights, taps, sems.at[0]),
        pltpu.make_async_copy(gain, gains, sems.at[1]),
    ]
    sources = [features.at[i] for i in range(3)] + [cotangent, long_filter]
    large = []
    for i, source in enumerate(sources):
        for y in range(SIDES[1]):
            target = out.at[:, y, :, pl.ds(i * EACH, EACH), :]
            large.append(pltpu.make_async_copy(source, target, sems.at[2 + 2 * i + y]))
    for copy in small + large:
        copy.start()
    for copy in small:
        copy.wait()
    first = (lax.axis_index("x") * SIDES[2] + lax.axis_index("c")) * EACH
    channels = gains.shape[1]
    shape = (EACH, channels)
    chosen = iota(shape, 1) == iota(shape, 0) + first
    for j in range(SUMS):
        line = gains[...] if j == 3 * TAPS else taps[j // TAPS, j % TAPS : j % TAPS + 1, :]
        line = jnp.broadcast_to(line, shape)
        column = jnp.sum(jnp.where(chosen, line, 0.0), axis=1, keepdims=True)
        table[j] = jnp.broadcast_to(column, (EACH, LANES))
    for copy in large:
        copy.wait()


def shifted_down(values, count):
    if count == 0:
        return values
    return jnp.where(iota(values.shape, 0) >= count, pltpu.roll(values, count, 0), 0.0)


def shifted_up(values, count):
    if count == 0:
        return values
    size = values.shape[0]
    return jnp.where(iota(values.shape, 0) < size - count, pltpu.roll(values, size - count, 0), 0.0)


def later(values, count, carry):
    if count == 0:
        return values
    turned = pltpu.roll(values, count, 1)
    return jnp.where(iota(values.shape, 1) >= count, turned, carry(turned, 1))


def earlier(values, count):
    if count == 0:
        return values
    turned = pltpu.roll(values, LANES - count, 1)
    return jnp.where(iota(values.shape, 1) < LANES - count, turned, shifted_up(turned, 1))


def fill_right(line_of, right, column):
    shape = (STEP, LANES)
    keep = iota(shape, 1) >= iota(shape, 0)
    before = jnp.zeros(shape, F32)
    for k in range(BLOCKS):
        line = jnp.broadcast_to(line_of(k), shape)
        turned = pltpu.roll(line, 0, 1, stride=1, stride_axis=0)
        part = jnp.where(keep, turned, before).astype(BF16)
        right[k * STEP : (k + 1) * STEP, column : column + LANES] = part
        before = turned


def left_rows(values, shifted):
    turned = [pltpu.roll(values, STEP * q, 1) if q else values for q in range(PHASES)]
    moved = [[shifted(turned[q], kk) for q in range(PHASES)] for kk in range(PHASES)]
    part = iota(values.shape, 1) // STEP
    rows = []
    for p in range(PHASES):
        base = moved[0][-p % PHASES]
        for kk in range(1, PHASES):
            base = jnp.where(part == kk, moved[kk][(kk - p) % PHASES], base)
        tiles = [shifted(base, PHASES * j).astype(BF16) for j in range(BLOCKS // PHASES)]
        rows.append(jnp.concatenate(tiles, axis=1))
    return rows


def joined(parts, carry):
    total = parts[0]
    for p in range(1, PHASES):
        total = total + later(parts[p], STEP * p, carry)
    return total


def middle_kernel(table, received, out, wide, packed, right, kept, mirrored, turned_back):
    wide[...] = received[...].astype(F32).reshape(BLOCKS * IN_ROWS, LANES)
    square = (LANES, LANES)
    mirror = jnp.where(iota(square, 0) + iota(square, 1) == LANES - 1, 1.0, 0.0).astype(BF16)

    def stream(i, c):
        return wide[pl.ds(i * EACH + c, BLOCKS, stride=IN_ROWS), :]

    def put(i, c, values):
        packed[pl.ds(i * EACH + c, BLOCKS, stride=OUT_ROWS), :] = values

    def weight(j, c):
        return table[j, c : c + 1, :]

    def rows(c):
        return slice(c * BLOCKS, (c + 1) * BLOCKS)

    PRIMED, MIXED, GATED, HISTORY, LONG = 0, 3, 4, 5, 11
    for c in range(EACH):
        primed = []
        for i in range(3):
            value = stream(i, c)
            running = weight(i * TAPS, c) * value
            for o in range(1, TAPS):
                moved = later(value, o, shifted_down)
                kept[HISTORY + 2 * i + o - 1, rows(c), :] = moved
                running = running + weight(i * TAPS + o, c) * moved
            kept[PRIMED + i, rows(c), :] = running
            primed.append(running)
        kept[MIXED, rows(c), :] = (primed[1] * primed[2]).astype(BF16).astype(F32)
        kept[GATED, rows(c), :] = (stream(3, c) * primed[0]).astype(BF16).astype(F32)
    mirrored[...] = jnp.dot(kept[GATED].astype(BF16), mirror, preferred_element_type=F32)
    half = EACH * BLOCKS
    for c in range(EACH):
        gain = weight(3 * TAPS, c)
        mixed = kept[MIXED, rows(c), :]
        gated = mirrored[rows(c), :]
        fill_right(lambda k: wide[k * IN_ROWS + 4 * EACH + c : k * IN_ROWS + 4 * EACH + c + 1, :], right.at[c], 0)
        fill_right(lambda k: kept[MIXED, c * BLOCKS + k : c * BLOCKS + k + 1, :], right.at[c], LANES)
        left = jnp.concatenate(left_rows(mixed, shifted_down) + left_rows(gated, shifted_up), axis=0)
        product = jnp.dot(left, right[c], preferred_element_type=F32)

        def parts(at, column):
            cut = slice(column, column + LANES)
            return [product[at + p * BLOCKS : at + (p + 1) * BLOCKS, cut] for p in range(PHASES)]

        conv = joined(parts(0, 0), shifted_down)
        corr = joined(parts(PHASES * BLOCKS, 0), shifted_up)
        cross = joined(parts(PHASES * BLOCKS, LANES), shifted_up)
        kept[LONG, rows(c), :] = (conv + gain * mixed).astype(BF16).astype(F32)
        turned_back[rows(c), :] = corr + gain * gated
        turned_back[half + c * BLOCKS : half + (c + 1) * BLOCKS, :] = cross
    turned_back[...] = jnp.dot(turned_back[...].astype(BF16), mirror, preferred_element_type=F32)
    sums = [[] for _ in range(SUMS)]
    for c in range(EACH):
        cot = stream(3, c)
        primed = [kept[PRIMED + i, rows(c), :] for i in range(3)]
        long_out = kept[LONG, rows(c), :]
        mixed_grad = turned_back[rows(c), :]
        primed_grad = [cot * long_out, mixed_grad * primed[2], mixed_grad * primed[1]]
        put(0, c, primed[0] * long_out)
        put(4, c, turned_back[half + c * BLOCKS : half + (c + 1) * BLOCKS, :])
        for i in range(3):
            running = weight(i * TAPS, c) * primed_grad[i]
            for o in range(1, TAPS):
                running = running + weight(i * TAPS + o, c) * earlier(primed_grad[i], o)
            put(1 + i, c, running)
            for o in range(TAPS):
                past = kept[HISTORY + 2 * i + o - 1, rows(c), :] if o else stream(i, c)
                sums[i * TAPS + o].append(jnp.sum(primed_grad[i] * past, axis=0, keepdims=True))
        both = kept[GATED, rows(c), :] * kept[MIXED, rows(c), :]
        sums[3 * TAPS].append(jnp.sum(both, axis=0, keepdims=True))
    stacked = jnp.concatenate([line for lines in sums for line in lines], axis=0)
    totals = jnp.sum(stacked, axis=1, keepdims=True)
    shape = stacked.shape
    line = jnp.sum(jnp.where(iota(shape, 0) == iota(shape, 1), totals, 0.0), axis=0, keepdims=True)
    left = jnp.broadcast_to(line, (BLOCKS, LANES))
    for r in range(IN_ROWS, OUT_ROWS):
        piece = left.astype(BF16).astype(F32)
        if r >= IN_ROWS + PIECES:
            piece = jnp.zeros_like(piece)
        left = left - piece
        packed[pl.ds(r, BLOCKS, stride=OUT_ROWS), :] = piece
    side = lax.axis_index("y")
    wanted = SIDES[2] * OUT_ROWS
    for x in range(SIDES[0]):
        at = pl.multiple_of((SIDES[1] * x + side) * wanted, 8)
        block = packed[pl.ds(at, wanted), :].astype(BF16)
        out[SIDES[2] * x : SIDES[2] * (x + 1)] = block.reshape(SIDES[2], OUT_ROWS, LANES)


def unpack_kernel(
    received, gated_out, feature_grad, long_grad, short_grad, skip_grad, taps, gains, sems
):
    targets = [gated_out] + [feature_grad.at[i] for i in range(3)] + [long_grad]
    copies = []
    for i, target in enumerate(targets):
        source = received.at[:, pl.ds(i * EACH, EACH), :]
        copies.append(pltpu.make_async_copy(source, target, sems.at[i]))
        copies[-1].start()
    pieces = received[:, IN_ROWS:OUT_ROWS, :].astype(F32)
    shape = (GROUPS, LANES)
    owner = jnp.where(iota(shape, 1) // EACH == iota(shape, 0), 1.0, 0.0).astype(BF16)
    total = jnp.zeros((LANES, LANES), F32)
    for p in range(PIECES):
        piece = pieces[:, p, :].astype(BF16)
        total = total + lax.dot_general(
            piece, owner, (((0,), (0,)), ((), ())), preferred_element_type=F32
        )
    total = total[: SUMS * EACH, :].reshape(SUMS, EACH, LANES)
    mine = iota(total.shape, 1) == iota(total.shape, 2) % EACH
    lines = jnp.sum(jnp.where(mine, total, 0.0), axis=1)
    channels = gains.shape[1]
    for i in range(3):
        taps[i] = lines[i * TAPS : (i + 1) * TAPS, 0:channels]
    gains[...] = lines[3 * TAPS :, 0:channels]
    last = [
        pltpu.make_async_copy(taps, short_grad, sems.at[STREAMS]),
        pltpu.make_async_copy(gains, skip_grad, sems.at[STREAMS + 1]),
    ]
    for copy in last:
        copy.start()
    for copy in copies + last:
        copy.wait()


def grant(mebibytes):
    return pltpu.CompilerParams(vmem_limit_bytes=mebibytes << 20)


def stay(array):
    return pltpu.with_memory_space_constraint(array, pltpu.HBM)


def shards(features, cotangent, long_filter, short_filters, skip_gain):
    channels = features.shape[1]
    whole = pl.BlockSpec(memory_space=pltpu.VMEM)
    far = pl.BlockSpec(memory_space=pltpu.HBM)
    cut = (SIDES[0], SIDES[2], EACH, LANES)
    parts, table = pl.pallas_call(
        pack_kernel,
        name="pack",
        compiler_params=grant(4),
        out_shape=(
            jax.ShapeDtypeStruct((*SIDES, IN_ROWS, LANES), BF16),
            jax.ShapeDtypeStruct((SUMS, EACH, LANES), F32),
        ),
        in_specs=[far] * 5,
        out_specs=(whole, whole),
        scratch_shapes=[
            pltpu.VMEM((3, TAPS, channels), F32),
            pltpu.VMEM((1, channels), F32),
            pltpu.SemaphoreType.DMA((2 + 2 * STREAMS,)),
        ],
    )(
        stay(features.reshape(3, *cut)),
        stay(cotangent.reshape(cut)),
        stay(long_filter.reshape(cut)),
        stay(jnp.swapaxes(short_filters, 1, 2)),
        stay(skip_gain.reshape(1, channels)),
    )
    columns = lax.all_to_all(
        parts.reshape(BLOCKS, IN_ROWS, LANES), SEQ, split_axis=0, concat_axis=0, tiled=True
    )
    results = pl.pallas_call(
        middle_kernel,
        name="middle",
        compiler_params=grant(12),
        out_shape=jax.ShapeDtypeStruct((GROUPS, OUT_ROWS, LANES), BF16),
        in_specs=[whole, whole],
        out_specs=whole,
        scratch_shapes=[
            pltpu.VMEM((BLOCKS * IN_ROWS, LANES), F32),
            pltpu.VMEM((BLOCKS * OUT_ROWS, LANES), F32),
            pltpu.VMEM((EACH, BLOCKS * STEP, 2 * LANES), BF16),
            pltpu.VMEM((12, EACH * BLOCKS, LANES), F32),
            pltpu.VMEM((EACH * BLOCKS, LANES), F32),
            pltpu.VMEM((2 * EACH * BLOCKS, LANES), F32),
        ],
    )(table, columns)
    back = lax.all_to_all(results, OWNERS, split_axis=0, concat_axis=0, tiled=True)
    block = (GROUPS, EACH, LANES)
    gated_out, feature_grad, long_grad, short_grad, skip_grad = pl.pallas_call(
        unpack_kernel,
        name="unpack",
        compiler_params=grant(4),
        out_shape=(
            jax.ShapeDtypeStruct(block, BF16),
            jax.ShapeDtypeStruct((3, *block), BF16),
            jax.ShapeDtypeStruct(block, BF16),
            jax.ShapeDtypeStruct((3, TAPS, channels), F32),
            jax.ShapeDtypeStruct((1, channels), F32),
        ),
        in_specs=[whole],
        out_specs=(far,) * 5,
        scratch_shapes=[
            pltpu.VMEM((3, TAPS, channels), F32),
            pltpu.VMEM((1, channels), F32),
            pltpu.SemaphoreType.DMA((STREAMS + 2,)),
        ],
    )(back)
    return (
        gated_out.reshape(channels, LANES),
        feature_grad.reshape(3, channels, LANES),
        long_grad.reshape(channels, LANES),
        jnp.swapaxes(short_grad, 1, 2),
        skip_grad.reshape(channels),
    )


def solution(mesh):
    torus = Mesh(mesh.devices.reshape(*SIDES, mesh.shape["chan"]), (*SEQ, "chan"))
    return jax.shard_map(
        shards,
        mesh=torus,
        in_specs=(
            P(None, "chan", SEQ),
            P("chan", SEQ),
            P("chan", SEQ),
            P(None, "chan", None),
            P("chan"),
        ),
        out_specs=(
            P("chan", SEQ),
            P(None, "chan", SEQ),
            P("chan", SEQ),
            P(None, "chan", None),
            P("chan"),
        ),
        check_vma=False,
    )
```

```python
import jax
import jax.numpy as jnp
from jax import lax
from jax.experimental import pallas as pl
from jax.experimental.pallas import tpu as pltpu
from jax.sharding import Mesh
from jax.sharding import PartitionSpec as P

SEQ = ("x", "y", "c")
SIDES = (4, 2, 2)
OWNERS = ("x", "c")
BLOCKS = 16
GROUPS = 8
EACH = 8
LANES = 128
STREAMS = 5
TAPS = 3
SUMS = 3 * TAPS + 1
IN_ROWS = STREAMS * EACH
OUT_ROWS = IN_ROWS + 16
PHASES = 4
STEP = LANES // PHASES
PAD = 8
BUFFERS = 8
SPLIT = 8

F32 = jnp.float32
BF16 = jnp.bfloat16


def iota(shape, dim):
    return lax.broadcasted_iota(jnp.int32, shape, dim)


def pack_kernel(features, cotangent, long_filter, weights, gain, out, table, taps, gains, sems):
    small = [
        pltpu.make_async_copy(weights, taps, sems.at[0]),
        pltpu.make_async_copy(gain, gains, sems.at[1]),
    ]
    sources = [features.at[i] for i in range(3)] + [cotangent, long_filter]
    large = []
    for i, source in enumerate(sources):
        for y in range(SIDES[1]):
            target = out.at[:, y, :, pl.ds(i * EACH, EACH), :]
            large.append(pltpu.make_async_copy(source, target, sems.at[2 + 2 * i + y]))
    for copy in small + large:
        copy.start()
    for copy in small:
        copy.wait()
    first = (lax.axis_index("x") * SIDES[2] + lax.axis_index("c")) * EACH
    channels = gains.shape[1]
    shape = (EACH, channels)
    chosen = iota(shape, 1) == iota(shape, 0) + first
    for j in range(SUMS):
        line = gains[...] if j == 3 * TAPS else taps[j // TAPS, j % TAPS : j % TAPS + 1, :]
        line = jnp.broadcast_to(line, shape)
        column = jnp.sum(jnp.where(chosen, line, 0.0), axis=1, keepdims=True)
        table[j] = jnp.broadcast_to(column, (EACH, LANES))
    for copy in large:
        copy.wait()


def after(values, before, count):
    mixed = jnp.where(iota(values.shape, 1) < LANES - count, values, before)
    return pltpu.roll(mixed, count, 1)


def ahead(values, behind, count):
    mixed = jnp.where(iota(values.shape, 1) >= count, values, behind)
    return pltpu.roll(mixed, LANES - count, 1)


def fill_right(line_of, right):
    shape = (STEP, LANES)
    keep = iota(shape, 1) >= iota(shape, 0)
    before = jnp.zeros(shape, F32)
    for k in range(BLOCKS):
        line = jnp.broadcast_to(line_of(k), shape)
        turned = pltpu.roll(line, 0, 1, stride=1, stride_axis=0)
        part = jnp.where(keep, turned, before).astype(BF16)
        right[k * STEP : (k + 1) * STEP, :] = part
        before = turned


class Slide:
    def __init__(self, ref, down):
        self.ref, self.down = ref, down

    def clear(self):
        at = 0 if self.down else BLOCKS
        self.ref[at : at + PAD, :] = jnp.zeros((PAD, LANES), F32)

    def put(self, values):
        at = PAD if self.down else 0
        self.ref[at : at + BLOCKS, :] = values

    def read(self, count):
        at = PAD - count if self.down else count
        return self.ref[at : at + BLOCKS, :]


def left_rows(values, turned, based):
    for q in range(PHASES):
        turned[q].put(pltpu.roll(values, STEP * q, 1) if q else values)
    moved = [[turned[q].read(kk) for q in range(PHASES)] for kk in range(PHASES)]
    part = iota(values.shape, 1) // STEP
    zero = jnp.zeros((PAD, LANES), F32)
    rows = []
    for p in range(PHASES):
        base = moved[0][-p % PHASES]
        for kk in range(1, PHASES):
            base = jnp.where(part == kk, moved[kk][(kk - p) % PHASES], base)
        based[p].put(base)
        tiles = [base, based[p].read(PHASES)]
        for tile in tiles[:2]:
            if based[p].down:
                tiles.append(jnp.concatenate([zero, tile[:PAD]], axis=0))
            else:
                tiles.append(jnp.concatenate([tile[PAD:], zero], axis=0))
        rows.append(jnp.concatenate([tile.astype(BF16) for tile in tiles], axis=1))
    return rows


def joined(parts, slides):
    total = parts[0]
    for p in range(1, PHASES):
        slides[p - 1].put(parts[p])
        total = total + after(parts[p], slides[p - 1].read(1), STEP * p)
    return total


def middle_kernel(
    table, received, out, wide, packed, right, kept, mirrored, turned_back, turn, base, piece, grad
):
    pad = jnp.zeros((IN_ROWS, LANES), F32)
    wide[0:IN_ROWS, :] = pad
    wide[(BLOCKS + 1) * IN_ROWS : (BLOCKS + 2) * IN_ROWS, :] = pad
    wide[IN_ROWS : (BLOCKS + 1) * IN_ROWS, :] = (
        received[...].astype(F32).reshape(BLOCKS * IN_ROWS, LANES)
    )
    square = (LANES, LANES)
    mirror = jnp.where(iota(square, 0) + iota(square, 1) == LANES - 1, 1.0, 0.0).astype(BF16)

    def stream(i, c, back=0):
        at = (1 - back) * IN_ROWS + i * EACH + c
        return wide[pl.ds(at, BLOCKS, stride=IN_ROWS), :]

    def put(i, c, values):
        packed[pl.ds(i * EACH + c, BLOCKS, stride=IN_ROWS), :] = values

    def weight(j, c):
        return table[j, c : c + 1, :]

    def rows(c):
        return slice(c * BLOCKS, (c + 1) * BLOCKS)

    def slides(ref, buffer, down):
        return [Slide(ref.at[buffer, n], d) for n, d in enumerate(down)]

    signals = [True] * PHASES + [False] * PHASES
    pieces = [True] * (PHASES - 1) + [False] * (2 * (PHASES - 1))
    turns = [slides(turn, n, signals) for n in range(BUFFERS)]
    bases = [slides(base, n, signals) for n in range(BUFFERS)]
    splits = [slides(piece, n, pieces) for n in range(BUFFERS)]
    grads = [slides(grad, n, [False] * 3) for n in range(BUFFERS)]
    for group in (turns, bases, splits, grads):
        for line in group:
            for slide in line:
                slide.clear()

    PRIMED, MIXED, GATED, HISTORY, LONG = 0, 3, 4, 5, 11
    for c in range(EACH):
        primed = []
        for i in range(3):
            value, before = stream(i, c), stream(i, c, 1)
            running = weight(i * TAPS, c) * value
            for o in range(1, TAPS):
                moved = after(value, before, o)
                kept[HISTORY + 2 * i + o - 1, rows(c), :] = moved
                running = running + weight(i * TAPS + o, c) * moved
            kept[PRIMED + i, rows(c), :] = running
            primed.append(running)
        kept[MIXED, rows(c), :] = (primed[1] * primed[2]).astype(BF16).astype(F32)
        kept[GATED, rows(c), :] = (stream(3, c) * primed[0]).astype(BF16).astype(F32)
    half = EACH * BLOCKS
    for n in range(SPLIT):
        cut = slice(n * half // SPLIT, (n + 1) * half // SPLIT)
        turned = jnp.dot(kept[GATED, cut, :].astype(BF16), mirror, preferred_element_type=F32)
        mirrored[cut, :] = turned
    for c in range(EACH):
        gain = weight(3 * TAPS, c)
        mixed = kept[MIXED, rows(c), :]
        gated = mirrored[rows(c), :]
        at = IN_ROWS + 4 * EACH + c
        fill_right(lambda k: wide[at + k * IN_ROWS : at + k * IN_ROWS + 1, :], right.at[c, 0])
        fill_right(
            lambda k: kept[MIXED, c * BLOCKS + k : c * BLOCKS + k + 1, :], right.at[c, 1]
        )
        turned, based, split = turns[c % BUFFERS], bases[c % BUFFERS], splits[c % BUFFERS]
        left = left_rows(mixed, turned[:PHASES], based[:PHASES])
        left += left_rows(gated, turned[PHASES:], based[PHASES:])
        product = jnp.dot(
            jnp.concatenate(left, axis=0),
            jnp.concatenate([right[c, 0], right[c, 1]], axis=1),
            preferred_element_type=F32,
        )

        def parts(first, column):
            cut = slice(column, column + LANES)
            lines = [first + p * BLOCKS for p in range(PHASES)]
            return [product[line : line + BLOCKS, cut] for line in lines]

        each = PHASES - 1
        conv = joined(parts(0, 0), split[:each])
        corr = joined(parts(PHASES * BLOCKS, 0), split[each : 2 * each])
        cross = joined(parts(PHASES * BLOCKS, LANES), split[2 * each :])
        kept[LONG, rows(c), :] = (conv + gain * mixed).astype(BF16).astype(F32)
        turned_back[rows(c), :] = corr + gain * gated
        turned_back[half + c * BLOCKS : half + (c + 1) * BLOCKS, :] = cross
    for n in range(SPLIT):
        for start in (0, half):
            cut = slice(start + n * half // SPLIT, start + (n + 1) * half // SPLIT)
            lines = turned_back[cut, :].astype(BF16)
            turned_back[cut, :] = jnp.dot(lines, mirror, preferred_element_type=F32)
    sums = [[] for _ in range(SUMS)]
    for c in range(EACH):
        cot = stream(3, c)
        primed = [kept[PRIMED + i, rows(c), :] for i in range(3)]
        long_out = kept[LONG, rows(c), :]
        mixed_grad = turned_back[rows(c), :]
        primed_grad = [cot * long_out, mixed_grad * primed[2], mixed_grad * primed[1]]
        put(0, c, primed[0] * long_out)
        put(4, c, turned_back[half + c * BLOCKS : half + (c + 1) * BLOCKS, :])
        for i in range(3):
            slide = grads[c % BUFFERS][i]
            slide.put(primed_grad[i])
            behind = slide.read(1)
            running = weight(i * TAPS, c) * primed_grad[i]
            for o in range(1, TAPS):
                running = running + weight(i * TAPS + o, c) * ahead(primed_grad[i], behind, o)
            put(1 + i, c, running)
            for o in range(TAPS):
                past = kept[HISTORY + 2 * i + o - 1, rows(c), :] if o else stream(i, c)
                sums[i * TAPS + o].append(jnp.sum(primed_grad[i] * past, axis=0, keepdims=True))
        both = kept[GATED, rows(c), :] * kept[MIXED, rows(c), :]
        sums[3 * TAPS].append(jnp.sum(both, axis=0, keepdims=True))
    stacked = jnp.concatenate([line for lines in sums for line in lines], axis=0)
    totals = jnp.sum(stacked, axis=1, keepdims=True)
    upper = totals.astype(BF16).astype(F32)
    shape = (SUMS, EACH, LANES)
    upper = jnp.broadcast_to(upper, stacked.shape).reshape(shape)
    totals = jnp.broadcast_to(totals, stacked.shape).reshape(shape)
    channels = GROUPS * EACH
    lane = iota(shape, 2)
    first = (lax.axis_index("x") * SIDES[2] + lax.axis_index("c")) * EACH
    both = jnp.where(lane < channels, upper, totals - upper)
    mine = lane % channels == iota(shape, 1) + first
    lines = jnp.sum(jnp.where(mine, both, 0.0), axis=1)
    rest = jnp.zeros((OUT_ROWS - IN_ROWS - SUMS, LANES), F32)
    lines = jnp.concatenate([lines, rest], axis=0).astype(BF16)
    side = lax.axis_index("y")
    wanted = SIDES[2] * IN_ROWS
    for x in range(SIDES[0]):
        at = pl.multiple_of((SIDES[1] * x + side) * wanted, 8)
        block = packed[pl.ds(at, wanted), :].astype(BF16)
        target = slice(SIDES[2] * x, SIDES[2] * (x + 1))
        out[target, 0:IN_ROWS, :] = block.reshape(SIDES[2], IN_ROWS, LANES)
    for n in range(GROUPS):
        out[n, IN_ROWS:OUT_ROWS, :] = lines


def unpack_kernel(
    received, gated_out, feature_grad, long_grad, short_grad, skip_grad, taps, gains, sems
):
    targets = [gated_out] + [feature_grad.at[i] for i in range(3)] + [long_grad]
    copies = []
    for i, target in enumerate(targets):
        source = received.at[:, pl.ds(i * EACH, EACH), :]
        copies.append(pltpu.make_async_copy(source, target, sems.at[i]))
        copies[-1].start()
    lines = jnp.sum(received[:, IN_ROWS:OUT_ROWS, :].astype(F32), axis=0)
    lines = lines + pltpu.roll(lines, LANES // 2, 1)
    channels = gains.shape[1]
    for i in range(3):
        taps[i] = lines[i * TAPS : (i + 1) * TAPS, 0:channels]
    gains[...] = lines[3 * TAPS : SUMS, 0:channels]
    last = [
        pltpu.make_async_copy(taps, short_grad, sems.at[STREAMS]),
        pltpu.make_async_copy(gains, skip_grad, sems.at[STREAMS + 1]),
    ]
    for copy in last:
        copy.start()
    for copy in copies + last:
        copy.wait()


def grant(mebibytes):
    return pltpu.CompilerParams(vmem_limit_bytes=mebibytes << 20)


def stay(array):
    return pltpu.with_memory_space_constraint(array, pltpu.HBM)


def shards(features, cotangent, long_filter, short_filters, skip_gain):
    channels = features.shape[1]
    whole = pl.BlockSpec(memory_space=pltpu.VMEM)
    far = pl.BlockSpec(memory_space=pltpu.HBM)
    cut = (SIDES[0], SIDES[2], EACH, LANES)
    parts, table = pl.pallas_call(
        pack_kernel,
        name="pack",
        compiler_params=grant(4),
        out_shape=(
            jax.ShapeDtypeStruct((*SIDES, IN_ROWS, LANES), BF16),
            jax.ShapeDtypeStruct((SUMS, EACH, LANES), F32),
        ),
        in_specs=[far] * 5,
        out_specs=(whole, whole),
        scratch_shapes=[
            pltpu.VMEM((3, TAPS, channels), F32),
            pltpu.VMEM((1, channels), F32),
            pltpu.SemaphoreType.DMA((2 + 2 * STREAMS,)),
        ],
    )(
        stay(features.reshape(3, *cut)),
        stay(cotangent.reshape(cut)),
        stay(long_filter.reshape(cut)),
        stay(jnp.swapaxes(short_filters, 1, 2)),
        stay(skip_gain.reshape(1, channels)),
    )
    columns = lax.all_to_all(
        parts.reshape(BLOCKS, IN_ROWS, LANES), SEQ, split_axis=0, concat_axis=0, tiled=True
    )
    results = pl.pallas_call(
        middle_kernel,
        name="middle",
        compiler_params=grant(12),
        out_shape=jax.ShapeDtypeStruct((GROUPS, OUT_ROWS, LANES), BF16),
        in_specs=[whole, whole],
        out_specs=whole,
        scratch_shapes=[
            pltpu.VMEM(((BLOCKS + 2) * IN_ROWS, LANES), F32),
            pltpu.VMEM((BLOCKS * IN_ROWS, LANES), F32),
            pltpu.VMEM((EACH, 2, BLOCKS * STEP, LANES), BF16),
            pltpu.VMEM((12, EACH * BLOCKS, LANES), F32),
            pltpu.VMEM((EACH * BLOCKS, LANES), F32),
            pltpu.VMEM((2 * EACH * BLOCKS, LANES), F32),
            pltpu.VMEM((BUFFERS, 2 * PHASES, BLOCKS + PAD, LANES), F32),
            pltpu.VMEM((BUFFERS, 2 * PHASES, BLOCKS + PAD, LANES), F32),
            pltpu.VMEM((BUFFERS, 3 * (PHASES - 1), BLOCKS + PAD, LANES), F32),
            pltpu.VMEM((BUFFERS, 3, BLOCKS + PAD, LANES), F32),
        ],
    )(table, columns)
    back = lax.all_to_all(results, OWNERS, split_axis=0, concat_axis=0, tiled=True)
    block = (GROUPS, EACH, LANES)
    gated_out, feature_grad, long_grad, short_grad, skip_grad = pl.pallas_call(
        unpack_kernel,
        name="unpack",
        compiler_params=grant(4),
        out_shape=(
            jax.ShapeDtypeStruct(block, BF16),
            jax.ShapeDtypeStruct((3, *block), BF16),
            jax.ShapeDtypeStruct(block, BF16),
            jax.ShapeDtypeStruct((3, TAPS, channels), F32),
            jax.ShapeDtypeStruct((1, channels), F32),
        ),
        in_specs=[whole],
        out_specs=(far,) * 5,
        scratch_shapes=[
            pltpu.VMEM((3, TAPS, channels), F32),
            pltpu.VMEM((1, channels), F32),
            pltpu.SemaphoreType.DMA((STREAMS + 2,)),
        ],
    )(back)
    return (
        gated_out.reshape(channels, LANES),
        feature_grad.reshape(3, channels, LANES),
        long_grad.reshape(channels, LANES),
        jnp.swapaxes(short_grad, 1, 2),
        skip_grad.reshape(channels),
    )


def solution(mesh):
    torus = Mesh(mesh.devices.reshape(*SIDES, mesh.shape["chan"]), (*SEQ, "chan"))
    return jax.shard_map(
        shards,
        mesh=torus,
        in_specs=(
            P(None, "chan", SEQ),
            P("chan", SEQ),
            P("chan", SEQ),
            P(None, "chan", None),
            P("chan"),
        ),
        out_specs=(
            P("chan", SEQ),
            P(None, "chan", SEQ),
            P("chan", SEQ),
            P(None, "chan", None),
            P("chan"),
        ),
        check_vma=False,
    )
```

```python
import jax
import jax.numpy as jnp
from jax import lax
from jax.experimental import pallas as pl
from jax.experimental.pallas import tpu as pltpu
from jax.sharding import Mesh
from jax.sharding import PartitionSpec as P

SEQ = ("x", "y", "c")
SIDES = (4, 2, 2)
OWNERS = ("x", "c")
BLOCKS = 16
GROUPS = 8
EACH = 8
LANES = 128
STREAMS = 5
TAPS = 3
SUMS = 3 * TAPS + 1
IN_ROWS = STREAMS * EACH
OUT_ROWS = IN_ROWS + 16
PHASES = 4
STEP = LANES // PHASES

F32 = jnp.float32
BF16 = jnp.bfloat16


def iota(shape, dim):
    return lax.broadcasted_iota(jnp.int32, shape, dim)


def pack_kernel(features, cotangent, long_filter, weights, gain, out, table, taps, gains, sems):
    small = [
        pltpu.make_async_copy(weights, taps, sems.at[0]),
        pltpu.make_async_copy(gain, gains, sems.at[1]),
    ]
    sources = [features.at[i] for i in range(3)] + [cotangent, long_filter]
    large = []
    for i, source in enumerate(sources):
        for y in range(SIDES[1]):
            target = out.at[:, y, :, pl.ds(i * EACH, EACH), :]
            large.append(pltpu.make_async_copy(source, target, sems.at[2 + 2 * i + y]))
    for copy in small + large:
        copy.start()
    for copy in small:
        copy.wait()
    first = (lax.axis_index("x") * SIDES[2] + lax.axis_index("c")) * EACH
    channels = gains.shape[1]
    shape = (EACH, channels)
    chosen = iota(shape, 1) == iota(shape, 0) + first
    for j in range(SUMS):
        line = gains[...] if j == 3 * TAPS else taps[j // TAPS, j % TAPS : j % TAPS + 1, :]
        line = jnp.broadcast_to(line, shape)
        column = jnp.sum(jnp.where(chosen, line, 0.0), axis=1, keepdims=True)
        table[j] = jnp.broadcast_to(column, (EACH, LANES))
    for copy in large:
        copy.wait()


def after(values, before, count):
    mixed = jnp.where(iota(values.shape, 1) < LANES - count, values, before)
    return pltpu.roll(mixed, count, 1)


def ahead(values, behind, count):
    mixed = jnp.where(iota(values.shape, 1) >= count, values, behind)
    return pltpu.roll(mixed, LANES - count, 1)


def fill_right(line_of, right):
    shape = (STEP, LANES)
    keep = iota(shape, 1) >= iota(shape, 0)
    before = jnp.zeros(shape, F32)
    for k in range(BLOCKS):
        line = jnp.broadcast_to(line_of(k), shape)
        turned = pltpu.roll(line, 0, 1, stride=1, stride_axis=0)
        part = jnp.where(keep, turned, before).astype(BF16)
        right[k * STEP : (k + 1) * STEP, :] = part
        before = turned


def shifted_down(values, count):
    if count == 0:
        return values
    whole, rest = divmod(count, 8)
    parts = [values[n : n + 8] for n in range(0, values.shape[0], 8)]
    zero = jnp.zeros_like(parts[0])
    if rest:
        keep = iota(zero.shape, 0) >= rest
        turned = [pltpu.roll(part, rest, 0) for part in parts]
        parts = [jnp.where(keep, t, b) for t, b in zip(turned, [zero] + turned[:-1])]
    return jnp.concatenate([zero] * whole + parts[: len(parts) - whole], axis=0)


def shifted_up(values, count):
    if count == 0:
        return values
    whole, rest = divmod(count, 8)
    parts = [values[n : n + 8] for n in range(0, values.shape[0], 8)]
    zero = jnp.zeros_like(parts[0])
    if rest:
        keep = iota(zero.shape, 0) < 8 - rest
        turned = [pltpu.roll(part, 8 - rest, 0) for part in parts]
        parts = [jnp.where(keep, t, b) for t, b in zip(turned, turned[1:] + [zero])]
    return jnp.concatenate(parts[whole:] + [zero] * whole, axis=0)


def left_rows(values, shifted):
    turned = [pltpu.roll(values, STEP * q, 1) if q else values for q in range(PHASES)]
    moved = [[shifted(turned[q], kk) for q in range(PHASES)] for kk in range(PHASES)]
    part = iota(values.shape, 1) // STEP
    rows = []
    for p in range(PHASES):
        base = moved[0][-p % PHASES]
        for kk in range(1, PHASES):
            base = jnp.where(part == kk, moved[kk][(kk - p) % PHASES], base)
        tiles = [shifted(base, PHASES * j).astype(BF16) for j in range(BLOCKS // PHASES)]
        rows.append(jnp.concatenate(tiles, axis=1))
    return rows


def joined(parts, shifted):
    total = parts[0]
    for p in range(1, PHASES):
        total = total + after(parts[p], shifted(parts[p], 1), STEP * p)
    return total


def middle_kernel(
    table, received, out, wide, packed, right, kept, mirrored, turned_back, left, product
):
    pad = jnp.zeros((IN_ROWS, LANES), F32)
    wide[0:IN_ROWS, :] = pad
    wide[(BLOCKS + 1) * IN_ROWS : (BLOCKS + 2) * IN_ROWS, :] = pad
    wide[IN_ROWS : (BLOCKS + 1) * IN_ROWS, :] = (
        received[...].astype(F32).reshape(BLOCKS * IN_ROWS, LANES)
    )
    square = (LANES, LANES)
    mirror = jnp.where(iota(square, 0) + iota(square, 1) == LANES - 1, 1.0, 0.0).astype(BF16)

    def stream(i, c, back=0):
        at = (1 - back) * IN_ROWS + i * EACH + c
        return wide[pl.ds(at, BLOCKS, stride=IN_ROWS), :]

    def put(i, c, values):
        packed[pl.ds(i * EACH + c, BLOCKS, stride=IN_ROWS), :] = values

    def weight(j, c):
        return table[j, c : c + 1, :]

    def rows(c):
        return slice(c * BLOCKS, (c + 1) * BLOCKS)

    PRIMED, MIXED, GATED, HISTORY, LONG = 0, 3, 4, 5, 11
    half = EACH * BLOCKS
    sums = [[] for _ in range(SUMS)]

    def prime(c):
        primed = []
        for i in range(3):
            value, before = stream(i, c), stream(i, c, 1)
            running = weight(i * TAPS, c) * value
            for o in range(1, TAPS):
                moved = after(value, before, o)
                kept[HISTORY + 2 * i + o - 1, rows(c), :] = moved
                running = running + weight(i * TAPS + o, c) * moved
            kept[PRIMED + i, rows(c), :] = running
            primed.append(running)
        kept[MIXED, rows(c), :] = (primed[1] * primed[2]).astype(BF16).astype(F32)
        kept[GATED, rows(c), :] = (stream(3, c) * primed[0]).astype(BF16).astype(F32)

    def reflect(ref, start, values):
        ref[start : start + BLOCKS, :] = jnp.dot(
            values.astype(BF16), mirror, preferred_element_type=F32
        )

    def filter_band(c):
        at = IN_ROWS + 4 * EACH + c
        fill_right(lambda k: wide[at + k * IN_ROWS : at + k * IN_ROWS + 1, :], right.at[c, 0])

    def mixed_band(c):
        at = c * BLOCKS
        fill_right(lambda k: kept[MIXED, at + k : at + k + 1, :], right.at[c, 1])

    def turn(c):
        reflect(mirrored, c * BLOCKS, kept[GATED, rows(c), :])

    def mixed_rows(c):
        lines = left_rows(kept[MIXED, rows(c), :], shifted_down)
        left[c, 0 : PHASES * BLOCKS, :] = jnp.concatenate(lines, axis=0)

    def gated_rows(c):
        lines = left_rows(mirrored[rows(c), :], shifted_up)
        left[c, PHASES * BLOCKS :, :] = jnp.concatenate(lines, axis=0)

    def multiply(c):
        band = jnp.concatenate([right[c, 0], right[c, 1]], axis=1)
        product[c] = jnp.dot(left[c], band, preferred_element_type=F32)

    def parts(c, first, column):
        lines = [first + p * BLOCKS for p in range(PHASES)]
        return [product[c, n : n + BLOCKS, column : column + LANES] for n in lines]

    def gather(c):
        gain = weight(3 * TAPS, c)
        conv = joined(parts(c, 0, 0), shifted_down)
        corr = joined(parts(c, PHASES * BLOCKS, 0), shifted_up)
        cross = joined(parts(c, PHASES * BLOCKS, LANES), shifted_up)
        kept[LONG, rows(c), :] = (conv + gain * kept[MIXED, rows(c), :]).astype(BF16).astype(F32)
        turned_back[rows(c), :] = corr + gain * mirrored[rows(c), :]
        turned_back[half + c * BLOCKS : half + (c + 1) * BLOCKS, :] = cross

    def turn_back(c):
        for start in (c * BLOCKS, half + c * BLOCKS):
            reflect(turned_back, start, turned_back[start : start + BLOCKS, :])

    def finish(c):
        cot = stream(3, c)
        primed = [kept[PRIMED + i, rows(c), :] for i in range(3)]
        long_out = kept[LONG, rows(c), :]
        mixed_grad = turned_back[rows(c), :]
        primed_grad = [cot * long_out, mixed_grad * primed[2], mixed_grad * primed[1]]
        put(0, c, primed[0] * long_out)
        put(4, c, turned_back[half + c * BLOCKS : half + (c + 1) * BLOCKS, :])
        for i in range(3):
            behind = shifted_up(primed_grad[i], 1)
            running = weight(i * TAPS, c) * primed_grad[i]
            for o in range(1, TAPS):
                running = running + weight(i * TAPS + o, c) * ahead(primed_grad[i], behind, o)
            put(1 + i, c, running)
            for o in range(TAPS):
                past = kept[HISTORY + 2 * i + o - 1, rows(c), :] if o else stream(i, c)
                sums[i * TAPS + o].append(jnp.sum(primed_grad[i] * past, axis=0, keepdims=True))
        both = kept[GATED, rows(c), :] * kept[MIXED, rows(c), :]
        sums[3 * TAPS].append(jnp.sum(both, axis=0, keepdims=True))

    for c in range(EACH):
        prime(c)
    for c in range(EACH):
        turn(c)
    for c in range(EACH):
        filter_band(c)
        mixed_rows(c)
    for c in range(EACH):
        mixed_band(c)
        gated_rows(c)
    for c in range(EACH):
        multiply(c)
    for c in range(EACH):
        gather(c)
    for c in range(EACH):
        turn_back(c)
    for c in range(EACH):
        finish(c)
    stacked = jnp.concatenate([line for lines in sums for line in lines], axis=0)
    totals = jnp.sum(stacked, axis=1, keepdims=True)
    upper = totals.astype(BF16).astype(F32)
    shape = (SUMS, EACH, LANES)
    upper = jnp.broadcast_to(upper, stacked.shape).reshape(shape)
    totals = jnp.broadcast_to(totals, stacked.shape).reshape(shape)
    channels = GROUPS * EACH
    lane = iota(shape, 2)
    first = (lax.axis_index("x") * SIDES[2] + lax.axis_index("c")) * EACH
    both = jnp.where(lane < channels, upper, totals - upper)
    mine = lane % channels == iota(shape, 1) + first
    lines = jnp.sum(jnp.where(mine, both, 0.0), axis=1)
    rest = jnp.zeros((OUT_ROWS - IN_ROWS - SUMS, LANES), F32)
    lines = jnp.concatenate([lines, rest], axis=0).astype(BF16)
    side = lax.axis_index("y")
    wanted = SIDES[2] * IN_ROWS
    for x in range(SIDES[0]):
        at = pl.multiple_of((SIDES[1] * x + side) * wanted, 8)
        block = packed[pl.ds(at, wanted), :].astype(BF16)
        target = slice(SIDES[2] * x, SIDES[2] * (x + 1))
        out[target, 0:IN_ROWS, :] = block.reshape(SIDES[2], IN_ROWS, LANES)
    for n in range(GROUPS):
        out[n, IN_ROWS:OUT_ROWS, :] = lines


def unpack_kernel(
    received, gated_out, feature_grad, long_grad, short_grad, skip_grad, taps, gains, sems
):
    targets = [gated_out] + [feature_grad.at[i] for i in range(3)] + [long_grad]
    copies = []
    for i, target in enumerate(targets):
        source = received.at[:, pl.ds(i * EACH, EACH), :]
        copies.append(pltpu.make_async_copy(source, target, sems.at[i]))
        copies[-1].start()
    lines = jnp.sum(received[:, IN_ROWS:OUT_ROWS, :].astype(F32), axis=0)
    lines = lines + pltpu.roll(lines, LANES // 2, 1)
    channels = gains.shape[1]
    for i in range(3):
        taps[i] = lines[i * TAPS : (i + 1) * TAPS, 0:channels]
    gains[...] = lines[3 * TAPS : SUMS, 0:channels]
    last = [
        pltpu.make_async_copy(taps, short_grad, sems.at[STREAMS]),
        pltpu.make_async_copy(gains, skip_grad, sems.at[STREAMS + 1]),
    ]
    for copy in last:
        copy.start()
    for copy in copies + last:
        copy.wait()


def grant(mebibytes):
    return pltpu.CompilerParams(vmem_limit_bytes=mebibytes << 20)


def stay(array):
    return pltpu.with_memory_space_constraint(array, pltpu.HBM)


def shards(features, cotangent, long_filter, short_filters, skip_gain):
    channels = features.shape[1]
    whole = pl.BlockSpec(memory_space=pltpu.VMEM)
    far = pl.BlockSpec(memory_space=pltpu.HBM)
    cut = (SIDES[0], SIDES[2], EACH, LANES)
    parts, table = pl.pallas_call(
        pack_kernel,
        name="pack",
        compiler_params=grant(4),
        out_shape=(
            jax.ShapeDtypeStruct((*SIDES, IN_ROWS, LANES), BF16),
            jax.ShapeDtypeStruct((SUMS, EACH, LANES), F32),
        ),
        in_specs=[far] * 5,
        out_specs=(whole, whole),
        scratch_shapes=[
            pltpu.VMEM((3, TAPS, channels), F32),
            pltpu.VMEM((1, channels), F32),
            pltpu.SemaphoreType.DMA((2 + 2 * STREAMS,)),
        ],
    )(
        stay(features.reshape(3, *cut)),
        stay(cotangent.reshape(cut)),
        stay(long_filter.reshape(cut)),
        stay(jnp.swapaxes(short_filters, 1, 2)),
        stay(skip_gain.reshape(1, channels)),
    )
    columns = lax.all_to_all(
        parts.reshape(BLOCKS, IN_ROWS, LANES), SEQ, split_axis=0, concat_axis=0, tiled=True
    )
    results = pl.pallas_call(
        middle_kernel,
        name="middle",
        compiler_params=grant(12),
        out_shape=jax.ShapeDtypeStruct((GROUPS, OUT_ROWS, LANES), BF16),
        in_specs=[whole, whole],
        out_specs=whole,
        scratch_shapes=[
            pltpu.VMEM(((BLOCKS + 2) * IN_ROWS, LANES), F32),
            pltpu.VMEM((BLOCKS * IN_ROWS, LANES), F32),
            pltpu.VMEM((EACH, 2, BLOCKS * STEP, LANES), BF16),
            pltpu.VMEM((12, EACH * BLOCKS, LANES), F32),
            pltpu.VMEM((EACH * BLOCKS, LANES), F32),
            pltpu.VMEM((2 * EACH * BLOCKS, LANES), F32),
            pltpu.VMEM((EACH, 2 * PHASES * BLOCKS, BLOCKS * STEP), BF16),
            pltpu.VMEM((EACH, 2 * PHASES * BLOCKS, 2 * LANES), F32),
        ],
    )(table, columns)
    back = lax.all_to_all(results, OWNERS, split_axis=0, concat_axis=0, tiled=True)
    block = (GROUPS, EACH, LANES)
    gated_out, feature_grad, long_grad, short_grad, skip_grad = pl.pallas_call(
        unpack_kernel,
        name="unpack",
        compiler_params=grant(4),
        out_shape=(
            jax.ShapeDtypeStruct(block, BF16),
            jax.ShapeDtypeStruct((3, *block), BF16),
            jax.ShapeDtypeStruct(block, BF16),
            jax.ShapeDtypeStruct((3, TAPS, channels), F32),
            jax.ShapeDtypeStruct((1, channels), F32),
        ),
        in_specs=[whole],
        out_specs=(far,) * 5,
        scratch_shapes=[
            pltpu.VMEM((3, TAPS, channels), F32),
            pltpu.VMEM((1, channels), F32),
            pltpu.SemaphoreType.DMA((STREAMS + 2,)),
        ],
    )(back)
    return (
        gated_out.reshape(channels, LANES),
        feature_grad.reshape(3, channels, LANES),
        long_grad.reshape(channels, LANES),
        jnp.swapaxes(short_grad, 1, 2),
        skip_grad.reshape(channels),
    )


def solution(mesh):
    torus = Mesh(mesh.devices.reshape(*SIDES, mesh.shape["chan"]), (*SEQ, "chan"))
    return jax.shard_map(
        shards,
        mesh=torus,
        in_specs=(
            P(None, "chan", SEQ),
            P("chan", SEQ),
            P("chan", SEQ),
            P(None, "chan", None),
            P("chan"),
        ),
        out_specs=(
            P("chan", SEQ),
            P(None, "chan", SEQ),
            P("chan", SEQ),
            P(None, "chan", None),
            P("chan"),
        ),
        check_vma=False,
    )
```

```python
import jax
import jax.numpy as jnp
from jax import lax
from jax.experimental import pallas as pl
from jax.experimental.pallas import tpu as pltpu
from jax.sharding import Mesh
from jax.sharding import PartitionSpec as P

SEQ = ("x", "y", "c")
SIDES = (4, 2, 2)
ENTRY = ("c", "y", "x")
OWNERS = ("c", "x")
BLOCKS = 16
GROUPS = 8
EACH = 8
LANES = 128
STREAMS = 5
TAPS = 3
SUMS = 3 * TAPS + 1
IN_ROWS = STREAMS * EACH
OUT_ROWS = IN_ROWS + 16
PHASES = 4
STEP = LANES // PHASES

F32 = jnp.float32
BF16 = jnp.bfloat16


def iota(shape, dim):
    return lax.broadcasted_iota(jnp.int32, shape, dim)


def pack_kernel(features, cotangent, long_filter, weights, gain, out, table, taps, gains, sems):
    small = [
        pltpu.make_async_copy(weights, taps, sems.at[0]),
        pltpu.make_async_copy(gain, gains, sems.at[1]),
    ]
    sources = [features.at[i] for i in range(3)] + [cotangent, long_filter]
    large = []
    for i, source in enumerate(sources):
        for y in range(SIDES[1]):
            target = out.at[:, y, :, pl.ds(i * EACH, EACH), :]
            large.append(pltpu.make_async_copy(source, target, sems.at[2 + 2 * i + y]))
    for copy in small + large:
        copy.start()
    for copy in small:
        copy.wait()
    first = (lax.axis_index("c") * SIDES[0] + lax.axis_index("x")) * EACH
    channels = gains.shape[1]
    shape = (EACH, channels)
    chosen = iota(shape, 1) == iota(shape, 0) + first
    for j in range(SUMS):
        line = gains[...] if j == 3 * TAPS else taps[j // TAPS, j % TAPS : j % TAPS + 1, :]
        line = jnp.broadcast_to(line, shape)
        column = jnp.sum(jnp.where(chosen, line, 0.0), axis=1, keepdims=True)
        table[j] = jnp.broadcast_to(column, (EACH, LANES))
    for copy in large:
        copy.wait()


def after(values, before, count):
    mixed = jnp.where(iota(values.shape, 1) < LANES - count, values, before)
    return pltpu.roll(mixed, count, 1)


def ahead(values, behind, count):
    mixed = jnp.where(iota(values.shape, 1) >= count, values, behind)
    return pltpu.roll(mixed, LANES - count, 1)


def fill_right(line_of, right):
    shape = (STEP, LANES)
    keep = iota(shape, 1) >= iota(shape, 0)
    before = jnp.zeros(shape, F32)
    for k in range(BLOCKS):
        line = jnp.broadcast_to(line_of(k), shape)
        turned = pltpu.roll(line, 0, 1, stride=1, stride_axis=0)
        part = jnp.where(keep, turned, before).astype(BF16)
        right[k * STEP : (k + 1) * STEP, :] = part
        before = turned


def shifted_down(values, count):
    if count == 0:
        return values
    whole, rest = divmod(count, 8)
    parts = [values[n : n + 8] for n in range(0, values.shape[0], 8)]
    zero = jnp.zeros_like(parts[0])
    if rest:
        keep = iota(zero.shape, 0) >= rest
        turned = [pltpu.roll(part, rest, 0) for part in parts]
        parts = [jnp.where(keep, t, b) for t, b in zip(turned, [zero] + turned[:-1])]
    return jnp.concatenate([zero] * whole + parts[: len(parts) - whole], axis=0)


def shifted_up(values, count):
    if count == 0:
        return values
    whole, rest = divmod(count, 8)
    parts = [values[n : n + 8] for n in range(0, values.shape[0], 8)]
    zero = jnp.zeros_like(parts[0])
    if rest:
        keep = iota(zero.shape, 0) < 8 - rest
        turned = [pltpu.roll(part, 8 - rest, 0) for part in parts]
        parts = [jnp.where(keep, t, b) for t, b in zip(turned, turned[1:] + [zero])]
    return jnp.concatenate(parts[whole:] + [zero] * whole, axis=0)


def left_rows(values, shifted):
    turned = [pltpu.roll(values, STEP * q, 1) if q else values for q in range(PHASES)]
    moved = [[shifted(turned[q], kk) for q in range(PHASES)] for kk in range(PHASES)]
    part = iota(values.shape, 1) // STEP
    rows = []
    for p in range(PHASES):
        base = moved[0][-p % PHASES]
        for kk in range(1, PHASES):
            base = jnp.where(part == kk, moved[kk][(kk - p) % PHASES], base)
        tiles = [shifted(base, PHASES * j).astype(BF16) for j in range(BLOCKS // PHASES)]
        rows.append(jnp.concatenate(tiles, axis=1))
    return rows


def joined(parts, shifted):
    total = parts[0]
    for p in range(1, PHASES):
        total = total + after(parts[p], shifted(parts[p], 1), STEP * p)
    return total


def middle_kernel(
    table, received, out, wide, packed, right, kept, mirrored, turned_back, left, product
):
    pad = jnp.zeros((IN_ROWS, LANES), F32)
    wide[0:IN_ROWS, :] = pad
    wide[(BLOCKS + 1) * IN_ROWS : (BLOCKS + 2) * IN_ROWS, :] = pad
    for c in range(SIDES[2]):
        for y in range(SIDES[1]):
            for x in range(SIDES[0]):
                source = (c * SIDES[1] + y) * SIDES[0] + x
                at = ((x * SIDES[1] + y) * SIDES[2] + c + 1) * IN_ROWS
                wide[at : at + IN_ROWS, :] = received[source].astype(F32)
    square = (LANES, LANES)
    mirror = jnp.where(iota(square, 0) + iota(square, 1) == LANES - 1, 1.0, 0.0).astype(BF16)

    def stream(i, c, back=0):
        at = (1 - back) * IN_ROWS + i * EACH + c
        return wide[pl.ds(at, BLOCKS, stride=IN_ROWS), :]

    def put(i, c, values):
        packed[pl.ds(i * EACH + c, BLOCKS, stride=IN_ROWS), :] = values

    def weight(j, c):
        return table[j, c : c + 1, :]

    def rows(c):
        return slice(c * BLOCKS, (c + 1) * BLOCKS)

    PRIMED, MIXED, GATED, HISTORY, LONG = 0, 3, 4, 5, 11
    half = EACH * BLOCKS
    sums = [[] for _ in range(SUMS)]

    def prime(c):
        primed = []
        for i in range(3):
            value, before = stream(i, c), stream(i, c, 1)
            running = weight(i * TAPS, c) * value
            for o in range(1, TAPS):
                moved = after(value, before, o)
                kept[HISTORY + 2 * i + o - 1, rows(c), :] = moved
                running = running + weight(i * TAPS + o, c) * moved
            kept[PRIMED + i, rows(c), :] = running
            primed.append(running)
        kept[MIXED, rows(c), :] = (primed[1] * primed[2]).astype(BF16).astype(F32)
        kept[GATED, rows(c), :] = (stream(3, c) * primed[0]).astype(BF16).astype(F32)

    def reflect(ref, start, values):
        ref[start : start + BLOCKS, :] = jnp.dot(
            values.astype(BF16), mirror, preferred_element_type=F32
        )

    def filter_band(c):
        at = IN_ROWS + 4 * EACH + c
        fill_right(lambda k: wide[at + k * IN_ROWS : at + k * IN_ROWS + 1, :], right.at[c, 0])

    def mixed_band(c):
        at = c * BLOCKS
        fill_right(lambda k: kept[MIXED, at + k : at + k + 1, :], right.at[c, 1])

    def turn(c):
        reflect(mirrored, c * BLOCKS, kept[GATED, rows(c), :])

    def mixed_rows(c):
        lines = left_rows(kept[MIXED, rows(c), :], shifted_down)
        left[c, 0 : PHASES * BLOCKS, :] = jnp.concatenate(lines, axis=0)

    def gated_rows(c):
        lines = left_rows(mirrored[rows(c), :], shifted_up)
        left[c, PHASES * BLOCKS :, :] = jnp.concatenate(lines, axis=0)

    def multiply(c):
        band = jnp.concatenate([right[c, 0], right[c, 1]], axis=1)
        product[c] = jnp.dot(left[c], band, preferred_element_type=F32)

    def parts(c, first, column):
        lines = [first + p * BLOCKS for p in range(PHASES)]
        return [product[c, n : n + BLOCKS, column : column + LANES] for n in lines]

    def gather(c):
        gain = weight(3 * TAPS, c)
        conv = joined(parts(c, 0, 0), shifted_down)
        corr = joined(parts(c, PHASES * BLOCKS, 0), shifted_up)
        cross = joined(parts(c, PHASES * BLOCKS, LANES), shifted_up)
        kept[LONG, rows(c), :] = (conv + gain * kept[MIXED, rows(c), :]).astype(BF16).astype(F32)
        turned_back[rows(c), :] = corr + gain * mirrored[rows(c), :]
        turned_back[half + c * BLOCKS : half + (c + 1) * BLOCKS, :] = cross

    def turn_back(c):
        for start in (c * BLOCKS, half + c * BLOCKS):
            reflect(turned_back, start, turned_back[start : start + BLOCKS, :])

    def finish(c):
        cot = stream(3, c)
        primed = [kept[PRIMED + i, rows(c), :] for i in range(3)]
        long_out = kept[LONG, rows(c), :]
        mixed_grad = turned_back[rows(c), :]
        primed_grad = [cot * long_out, mixed_grad * primed[2], mixed_grad * primed[1]]
        put(0, c, primed[0] * long_out)
        put(4, c, turned_back[half + c * BLOCKS : half + (c + 1) * BLOCKS, :])
        for i in range(3):
            behind = shifted_up(primed_grad[i], 1)
            running = weight(i * TAPS, c) * primed_grad[i]
            for o in range(1, TAPS):
                running = running + weight(i * TAPS + o, c) * ahead(primed_grad[i], behind, o)
            put(1 + i, c, running)
            for o in range(TAPS):
                past = kept[HISTORY + 2 * i + o - 1, rows(c), :] if o else stream(i, c)
                sums[i * TAPS + o].append(jnp.sum(primed_grad[i] * past, axis=0, keepdims=True))
        both = kept[GATED, rows(c), :] * kept[MIXED, rows(c), :]
        sums[3 * TAPS].append(jnp.sum(both, axis=0, keepdims=True))

    for c in range(EACH):
        prime(c)
    for c in range(EACH):
        turn(c)
    for c in range(EACH):
        filter_band(c)
        mixed_rows(c)
    for c in range(EACH):
        mixed_band(c)
        gated_rows(c)
    for c in range(EACH):
        multiply(c)
    for c in range(EACH):
        gather(c)
    for c in range(EACH):
        turn_back(c)
    for c in range(EACH):
        finish(c)
    stacked = jnp.concatenate([line for lines in sums for line in lines], axis=0)
    totals = jnp.sum(stacked, axis=1, keepdims=True)
    upper = totals.astype(BF16).astype(F32)
    shape = (SUMS, EACH, LANES)
    upper = jnp.broadcast_to(upper, stacked.shape).reshape(shape)
    totals = jnp.broadcast_to(totals, stacked.shape).reshape(shape)
    channels = GROUPS * EACH
    lane = iota(shape, 2)
    first = (lax.axis_index("c") * SIDES[0] + lax.axis_index("x")) * EACH
    both = jnp.where(lane < channels, upper, totals - upper)
    mine = lane % channels == iota(shape, 1) + first
    lines = jnp.sum(jnp.where(mine, both, 0.0), axis=1)
    rest = jnp.zeros((OUT_ROWS - IN_ROWS - SUMS, LANES), F32)
    lines = jnp.concatenate([lines, rest], axis=0).astype(BF16)
    side = lax.axis_index("y")
    for c in range(SIDES[2]):
        for x in range(SIDES[0]):
            block = (x * SIDES[1] + side) * SIDES[2] + c
            at = pl.multiple_of(block * IN_ROWS, 8)
            out[c * SIDES[0] + x, 0:IN_ROWS, :] = packed[pl.ds(at, IN_ROWS), :].astype(BF16)
    for n in range(GROUPS):
        out[n, IN_ROWS:OUT_ROWS, :] = lines


def unpack_kernel(
    received, gated_out, feature_grad, long_grad, short_grad, skip_grad, taps, gains, sems
):
    targets = [gated_out] + [feature_grad.at[i] for i in range(3)] + [long_grad]
    copies = []
    for i, target in enumerate(targets):
        source = received.at[:, pl.ds(i * EACH, EACH), :]
        copies.append(pltpu.make_async_copy(source, target, sems.at[i]))
        copies[-1].start()
    lines = jnp.sum(received[:, IN_ROWS:OUT_ROWS, :].astype(F32), axis=0)
    lines = lines + pltpu.roll(lines, LANES // 2, 1)
    channels = gains.shape[1]
    for i in range(3):
        taps[i] = lines[i * TAPS : (i + 1) * TAPS, 0:channels]
    gains[...] = lines[3 * TAPS : SUMS, 0:channels]
    last = [
        pltpu.make_async_copy(taps, short_grad, sems.at[STREAMS]),
        pltpu.make_async_copy(gains, skip_grad, sems.at[STREAMS + 1]),
    ]
    for copy in last:
        copy.start()
    for copy in copies + last:
        copy.wait()


def grant(mebibytes):
    return pltpu.CompilerParams(vmem_limit_bytes=mebibytes << 20)


def stay(array):
    return pltpu.with_memory_space_constraint(array, pltpu.HBM)


def shards(features, cotangent, long_filter, short_filters, skip_gain):
    channels = features.shape[1]
    whole = pl.BlockSpec(memory_space=pltpu.VMEM)
    far = pl.BlockSpec(memory_space=pltpu.HBM)
    cut = (SIDES[2], SIDES[0], EACH, LANES)
    parts, table = pl.pallas_call(
        pack_kernel,
        name="pack",
        compiler_params=grant(4),
        out_shape=(
            jax.ShapeDtypeStruct((*SIDES[::-1], IN_ROWS, LANES), BF16),
            jax.ShapeDtypeStruct((SUMS, EACH, LANES), F32),
        ),
        in_specs=[far] * 5,
        out_specs=(whole, whole),
        scratch_shapes=[
            pltpu.VMEM((3, TAPS, channels), F32),
            pltpu.VMEM((1, channels), F32),
            pltpu.SemaphoreType.DMA((2 + 2 * STREAMS,)),
        ],
    )(
        stay(features.reshape(3, *cut)),
        stay(cotangent.reshape(cut)),
        stay(long_filter.reshape(cut)),
        stay(jnp.swapaxes(short_filters, 1, 2)),
        stay(skip_gain.reshape(1, channels)),
    )
    columns = lax.all_to_all(
        parts.reshape(BLOCKS, IN_ROWS, LANES), ENTRY, split_axis=0, concat_axis=0, tiled=True
    )
    results = pl.pallas_call(
        middle_kernel,
        name="middle",
        compiler_params=grant(12),
        out_shape=jax.ShapeDtypeStruct((GROUPS, OUT_ROWS, LANES), BF16),
        in_specs=[whole, whole],
        out_specs=whole,
        scratch_shapes=[
            pltpu.VMEM(((BLOCKS + 2) * IN_ROWS, LANES), F32),
            pltpu.VMEM((BLOCKS * IN_ROWS, LANES), F32),
            pltpu.VMEM((EACH, 2, BLOCKS * STEP, LANES), BF16),
            pltpu.VMEM((12, EACH * BLOCKS, LANES), F32),
            pltpu.VMEM((EACH * BLOCKS, LANES), F32),
            pltpu.VMEM((2 * EACH * BLOCKS, LANES), F32),
            pltpu.VMEM((EACH, 2 * PHASES * BLOCKS, BLOCKS * STEP), BF16),
            pltpu.VMEM((EACH, 2 * PHASES * BLOCKS, 2 * LANES), F32),
        ],
    )(table, columns)
    back = lax.all_to_all(results, OWNERS, split_axis=0, concat_axis=0, tiled=True)
    block = (GROUPS, EACH, LANES)
    gated_out, feature_grad, long_grad, short_grad, skip_grad = pl.pallas_call(
        unpack_kernel,
        name="unpack",
        compiler_params=grant(4),
        out_shape=(
            jax.ShapeDtypeStruct(block, BF16),
            jax.ShapeDtypeStruct((3, *block), BF16),
            jax.ShapeDtypeStruct(block, BF16),
            jax.ShapeDtypeStruct((3, TAPS, channels), F32),
            jax.ShapeDtypeStruct((1, channels), F32),
        ),
        in_specs=[whole],
        out_specs=(far,) * 5,
        scratch_shapes=[
            pltpu.VMEM((3, TAPS, channels), F32),
            pltpu.VMEM((1, channels), F32),
            pltpu.SemaphoreType.DMA((STREAMS + 2,)),
        ],
    )(back)
    return (
        gated_out.reshape(channels, LANES),
        feature_grad.reshape(3, channels, LANES),
        long_grad.reshape(channels, LANES),
        jnp.swapaxes(short_grad, 1, 2),
        skip_grad.reshape(channels),
    )


def solution(mesh):
    torus = Mesh(mesh.devices.reshape(*SIDES, mesh.shape["chan"]), (*SEQ, "chan"))
    return jax.shard_map(
        shards,
        mesh=torus,
        in_specs=(
            P(None, "chan", SEQ),
            P("chan", SEQ),
            P("chan", SEQ),
            P(None, "chan", None),
            P("chan"),
        ),
        out_specs=(
            P("chan", SEQ),
            P(None, "chan", SEQ),
            P("chan", SEQ),
            P(None, "chan", None),
            P("chan"),
        ),
        check_vma=False,
    )
```

```python
import jax
import jax.numpy as jnp
from jax import lax
from jax.experimental import pallas as pl
from jax.experimental.pallas import tpu as pltpu
from jax.sharding import Mesh
from jax.sharding import PartitionSpec as P

SEQ = ("x", "y", "c")
SIDES = (4, 2, 2)
ENTRY = ("c", "y", "x")
OWNERS = ("c", "x")
BLOCKS = 16
GROUPS = 8
EACH = 8
LANES = 128
STREAMS = 5
TAPS = 3
SUMS = 3 * TAPS + 1
IN_ROWS = STREAMS * EACH
OUT_ROWS = IN_ROWS + 16
PHASES = 4
STEP = LANES // PHASES

F32 = jnp.float32
BF16 = jnp.bfloat16


def iota(shape, dim):
    return lax.broadcasted_iota(jnp.int32, shape, dim)


def pack_kernel(features, cotangent, long_filter, weights, gain, out, table, taps, gains, sems):
    small = [
        pltpu.make_async_copy(weights, taps, sems.at[0]),
        pltpu.make_async_copy(gain, gains, sems.at[1]),
    ]
    sources = [features.at[i] for i in range(3)] + [cotangent, long_filter]
    large = []
    for i, source in enumerate(sources):
        target = out.at[:, 0, :, pl.ds(i * EACH, EACH), :]
        large.append(pltpu.make_async_copy(source, target, sems.at[2 + i]))
    for copy in small + large:
        copy.start()
    for copy in small:
        copy.wait()
    first = (lax.axis_index("c") * SIDES[0] + lax.axis_index("x")) * EACH
    channels = gains.shape[1]
    shape = (EACH, channels)
    chosen = iota(shape, 1) == iota(shape, 0) + first
    for j in range(SUMS):
        line = gains[...] if j == 3 * TAPS else taps[j // TAPS, j % TAPS : j % TAPS + 1, :]
        line = jnp.broadcast_to(line, shape)
        column = jnp.sum(jnp.where(chosen, line, 0.0), axis=1, keepdims=True)
        table[j] = jnp.broadcast_to(column, (EACH, LANES))
    for copy in large:
        copy.wait()
    out[:, 1] = out[:, 0]


def after(values, before, count):
    mixed = jnp.where(iota(values.shape, 1) < LANES - count, values, before)
    return pltpu.roll(mixed, count, 1)


def ahead(values, behind, count):
    mixed = jnp.where(iota(values.shape, 1) >= count, values, behind)
    return pltpu.roll(mixed, LANES - count, 1)


def fill_right(line_of, right):
    shape = (STEP, LANES)
    keep = iota(shape, 1) >= iota(shape, 0)
    before = jnp.zeros(shape, F32)
    for k in range(BLOCKS):
        line = jnp.broadcast_to(line_of(k), shape)
        turned = pltpu.roll(line, 0, 1, stride=1, stride_axis=0)
        part = jnp.where(keep, turned, before).astype(BF16)
        right[k * STEP : (k + 1) * STEP, :] = part
        before = turned


def shifted_down(values, count):
    if count == 0:
        return values
    whole, rest = divmod(count, 8)
    parts = [values[n : n + 8] for n in range(0, values.shape[0], 8)]
    zero = jnp.zeros_like(parts[0])
    if rest:
        keep = iota(zero.shape, 0) >= rest
        turned = [pltpu.roll(part, rest, 0) for part in parts]
        parts = [jnp.where(keep, t, b) for t, b in zip(turned, [zero] + turned[:-1])]
    return jnp.concatenate([zero] * whole + parts[: len(parts) - whole], axis=0)


def shifted_up(values, count):
    if count == 0:
        return values
    whole, rest = divmod(count, 8)
    parts = [values[n : n + 8] for n in range(0, values.shape[0], 8)]
    zero = jnp.zeros_like(parts[0])
    if rest:
        keep = iota(zero.shape, 0) < 8 - rest
        turned = [pltpu.roll(part, 8 - rest, 0) for part in parts]
        parts = [jnp.where(keep, t, b) for t, b in zip(turned, turned[1:] + [zero])]
    return jnp.concatenate(parts[whole:] + [zero] * whole, axis=0)


def left_rows(values, shifted):
    turned = [pltpu.roll(values, STEP * q, 1) if q else values for q in range(PHASES)]
    moved = [[shifted(turned[q], kk) for q in range(PHASES)] for kk in range(PHASES)]
    part = iota(values.shape, 1) // STEP
    rows = []
    for p in range(PHASES):
        base = moved[0][-p % PHASES]
        for kk in range(1, PHASES):
            base = jnp.where(part == kk, moved[kk][(kk - p) % PHASES], base)
        tiles = [shifted(base, PHASES * j).astype(BF16) for j in range(BLOCKS // PHASES)]
        rows.append(jnp.concatenate(tiles, axis=1))
    return rows


def joined(parts, shifted):
    total = parts[0]
    for p in range(1, PHASES):
        total = total + after(parts[p], shifted(parts[p], 1), STEP * p)
    return total


def middle_kernel(
    table, received, out, wide, packed, right, kept, mirrored, turned_back, left, product, sums
):
    pad = jnp.zeros((IN_ROWS, LANES), F32)
    wide[0:IN_ROWS, :] = pad
    wide[(BLOCKS + 1) * IN_ROWS : (BLOCKS + 2) * IN_ROWS, :] = pad
    for c in range(SIDES[2]):
        for y in range(SIDES[1]):
            for x in range(SIDES[0]):
                source = (c * SIDES[1] + y) * SIDES[0] + x
                at = ((x * SIDES[1] + y) * SIDES[2] + c + 1) * IN_ROWS
                wide[at : at + IN_ROWS, :] = received[source].astype(F32)
    square = (LANES, LANES)
    mirror = jnp.where(iota(square, 0) + iota(square, 1) == LANES - 1, 1.0, 0.0).astype(BF16)

    def stream(i, c, back=0):
        at = (1 - back) * IN_ROWS + i * EACH + c
        return wide[pl.ds(at, BLOCKS, stride=IN_ROWS), :]

    def put(i, c, values):
        packed[pl.ds(i * EACH + c, BLOCKS, stride=IN_ROWS), :] = values

    def weight(j, c):
        return table[j, c : c + 1, :]

    def rows(c):
        return slice(c * BLOCKS, (c + 1) * BLOCKS)

    PRIMED, MIXED, GATED, HISTORY, LONG = 0, 3, 4, 5, 11
    half = EACH * BLOCKS

    def add(j, c, values):
        at = (j * EACH + c) * 8
        sums[at : at + 8, :] = values[0:8] + values[8:16]

    def prime(c):
        primed = []
        for i in range(3):
            value, before = stream(i, c), stream(i, c, 1)
            running = weight(i * TAPS, c) * value
            for o in range(1, TAPS):
                moved = after(value, before, o)
                kept[HISTORY + 2 * i + o - 1, rows(c), :] = moved
                running = running + weight(i * TAPS + o, c) * moved
            kept[PRIMED + i, rows(c), :] = running
            primed.append(running)
        kept[MIXED, rows(c), :] = (primed[1] * primed[2]).astype(BF16).astype(F32)
        kept[GATED, rows(c), :] = (stream(3, c) * primed[0]).astype(BF16).astype(F32)

    def reflect(ref, start, values):
        ref[start : start + BLOCKS, :] = jnp.dot(
            values.astype(BF16), mirror, preferred_element_type=F32
        )

    def filter_band(c):
        at = IN_ROWS + 4 * EACH + c
        fill_right(lambda k: wide[at + k * IN_ROWS : at + k * IN_ROWS + 1, :], right.at[c, 0])

    def mixed_band(c):
        at = c * BLOCKS
        fill_right(lambda k: kept[MIXED, at + k : at + k + 1, :], right.at[c, 1])

    def turn(c):
        reflect(mirrored, c * BLOCKS, kept[GATED, rows(c), :])

    def mixed_rows(c):
        lines = left_rows(kept[MIXED, rows(c), :], shifted_down)
        left[c, 0 : PHASES * BLOCKS, :] = jnp.concatenate(lines, axis=0)

    def gated_rows(c):
        lines = left_rows(mirrored[rows(c), :], shifted_up)
        left[c, PHASES * BLOCKS :, :] = jnp.concatenate(lines, axis=0)

    def multiply(c):
        band = jnp.concatenate([right[c, 0], right[c, 1]], axis=1)
        product[c] = jnp.dot(left[c], band, preferred_element_type=F32)

    def parts(c, first, column):
        lines = [first + p * BLOCKS for p in range(PHASES)]
        return [product[c, n : n + BLOCKS, column : column + LANES] for n in lines]

    def gather(c):
        gain = weight(3 * TAPS, c)
        conv = joined(parts(c, 0, 0), shifted_down)
        corr = joined(parts(c, PHASES * BLOCKS, 0), shifted_up)
        cross = joined(parts(c, PHASES * BLOCKS, LANES), shifted_up)
        kept[LONG, rows(c), :] = (conv + gain * kept[MIXED, rows(c), :]).astype(BF16).astype(F32)
        turned_back[rows(c), :] = corr + gain * mirrored[rows(c), :]
        turned_back[half + c * BLOCKS : half + (c + 1) * BLOCKS, :] = cross

    def turn_back(c):
        for start in (c * BLOCKS, half + c * BLOCKS):
            reflect(turned_back, start, turned_back[start : start + BLOCKS, :])

    def finish(c):
        cot = stream(3, c)
        primed = [kept[PRIMED + i, rows(c), :] for i in range(3)]
        long_out = kept[LONG, rows(c), :]
        mixed_grad = turned_back[rows(c), :]
        primed_grad = [cot * long_out, mixed_grad * primed[2], mixed_grad * primed[1]]
        put(0, c, primed[0] * long_out)
        put(4, c, turned_back[half + c * BLOCKS : half + (c + 1) * BLOCKS, :])
        for i in range(3):
            behind = shifted_up(primed_grad[i], 1)
            running = weight(i * TAPS, c) * primed_grad[i]
            for o in range(1, TAPS):
                running = running + weight(i * TAPS + o, c) * ahead(primed_grad[i], behind, o)
            put(1 + i, c, running)
            for o in range(TAPS):
                past = kept[HISTORY + 2 * i + o - 1, rows(c), :] if o else stream(i, c)
                add(i * TAPS + o, c, primed_grad[i] * past)
        add(3 * TAPS, c, kept[GATED, rows(c), :] * kept[MIXED, rows(c), :])

    for c in range(EACH):
        prime(c)
    for c in range(EACH):
        turn(c)
    for c in range(EACH):
        filter_band(c)
        mixed_rows(c)
    for c in range(EACH):
        mixed_band(c)
        gated_rows(c)
    for c in range(EACH):
        multiply(c)
    for c in range(EACH):
        gather(c)
    for c in range(EACH):
        turn_back(c)
    for c in range(EACH):
        finish(c)
    lines = []
    for j in range(SUMS):
        line = sums[pl.ds(j * EACH * 8, EACH, stride=8), :]
        for n in range(1, 8):
            line = line + sums[pl.ds(j * EACH * 8 + n, EACH, stride=8), :]
        lines.append(line)
    stacked = jnp.concatenate(lines, axis=0)
    totals = jnp.sum(stacked, axis=1, keepdims=True)
    upper = totals.astype(BF16).astype(F32)
    shape = (SUMS, EACH, LANES)
    upper = jnp.broadcast_to(upper, stacked.shape).reshape(shape)
    totals = jnp.broadcast_to(totals, stacked.shape).reshape(shape)
    channels = GROUPS * EACH
    lane = iota(shape, 2)
    first = (lax.axis_index("c") * SIDES[0] + lax.axis_index("x")) * EACH
    both = jnp.where(lane < channels, upper, totals - upper)
    mine = lane % channels == iota(shape, 1) + first
    lines = jnp.sum(jnp.where(mine, both, 0.0), axis=1)
    rest = jnp.zeros((OUT_ROWS - IN_ROWS - SUMS, LANES), F32)
    lines = jnp.concatenate([lines, rest], axis=0).astype(BF16)
    side = lax.axis_index("y")
    for c in range(SIDES[2]):
        for x in range(SIDES[0]):
            block = (x * SIDES[1] + side) * SIDES[2] + c
            at = pl.multiple_of(block * IN_ROWS, 8)
            out[c * SIDES[0] + x, 0:IN_ROWS, :] = packed[pl.ds(at, IN_ROWS), :].astype(BF16)
    for n in range(GROUPS):
        out[n, IN_ROWS:OUT_ROWS, :] = lines


def unpack_kernel(
    received, gated_out, feature_grad, long_grad, short_grad, skip_grad, taps, gains, sems
):
    targets = [gated_out] + [feature_grad.at[i] for i in range(3)] + [long_grad]
    copies = []
    for i, target in enumerate(targets):
        source = received.at[:, pl.ds(i * EACH, EACH), :]
        copies.append(pltpu.make_async_copy(source, target, sems.at[i]))
        copies[-1].start()
    lines = jnp.sum(received[:, IN_ROWS:OUT_ROWS, :].astype(F32), axis=0)
    lines = lines + pltpu.roll(lines, LANES // 2, 1)
    channels = gains.shape[1]
    for i in range(3):
        taps[i] = lines[i * TAPS : (i + 1) * TAPS, 0:channels]
    gains[...] = lines[3 * TAPS : SUMS, 0:channels]
    last = [
        pltpu.make_async_copy(taps, short_grad, sems.at[STREAMS]),
        pltpu.make_async_copy(gains, skip_grad, sems.at[STREAMS + 1]),
    ]
    for copy in last:
        copy.start()
    for copy in copies + last:
        copy.wait()


def grant(mebibytes):
    return pltpu.CompilerParams(vmem_limit_bytes=mebibytes << 20)


def stay(array):
    return pltpu.with_memory_space_constraint(array, pltpu.HBM)


def shards(features, cotangent, long_filter, short_filters, skip_gain):
    channels = features.shape[1]
    whole = pl.BlockSpec(memory_space=pltpu.VMEM)
    far = pl.BlockSpec(memory_space=pltpu.HBM)
    cut = (SIDES[2], SIDES[0], EACH, LANES)
    parts, table = pl.pallas_call(
        pack_kernel,
        name="pack",
        compiler_params=grant(4),
        out_shape=(
            jax.ShapeDtypeStruct((*SIDES[::-1], IN_ROWS, LANES), BF16),
            jax.ShapeDtypeStruct((SUMS, EACH, LANES), F32),
        ),
        in_specs=[far] * 5,
        out_specs=(whole, whole),
        scratch_shapes=[
            pltpu.VMEM((3, TAPS, channels), F32),
            pltpu.VMEM((1, channels), F32),
            pltpu.SemaphoreType.DMA((2 + STREAMS,)),
        ],
    )(
        stay(features.reshape(3, *cut)),
        stay(cotangent.reshape(cut)),
        stay(long_filter.reshape(cut)),
        stay(jnp.swapaxes(short_filters, 1, 2)),
        stay(skip_gain.reshape(1, channels)),
    )
    columns = lax.all_to_all(
        parts.reshape(BLOCKS, IN_ROWS, LANES), ENTRY, split_axis=0, concat_axis=0, tiled=True
    )
    results = pl.pallas_call(
        middle_kernel,
        name="middle",
        compiler_params=grant(12),
        out_shape=jax.ShapeDtypeStruct((GROUPS, OUT_ROWS, LANES), BF16),
        in_specs=[whole, whole],
        out_specs=whole,
        scratch_shapes=[
            pltpu.VMEM(((BLOCKS + 2) * IN_ROWS, LANES), F32),
            pltpu.VMEM((BLOCKS * IN_ROWS, LANES), F32),
            pltpu.VMEM((EACH, 2, BLOCKS * STEP, LANES), BF16),
            pltpu.VMEM((12, EACH * BLOCKS, LANES), F32),
            pltpu.VMEM((EACH * BLOCKS, LANES), F32),
            pltpu.VMEM((2 * EACH * BLOCKS, LANES), F32),
            pltpu.VMEM((EACH, 2 * PHASES * BLOCKS, BLOCKS * STEP), BF16),
            pltpu.VMEM((EACH, 2 * PHASES * BLOCKS, 2 * LANES), F32),
            pltpu.VMEM((SUMS * EACH * 8, LANES), F32),
        ],
    )(table, columns)
    back = lax.all_to_all(results, OWNERS, split_axis=0, concat_axis=0, tiled=True)
    block = (GROUPS, EACH, LANES)
    gated_out, feature_grad, long_grad, short_grad, skip_grad = pl.pallas_call(
        unpack_kernel,
        name="unpack",
        compiler_params=grant(4),
        out_shape=(
            jax.ShapeDtypeStruct(block, BF16),
            jax.ShapeDtypeStruct((3, *block), BF16),
            jax.ShapeDtypeStruct(block, BF16),
            jax.ShapeDtypeStruct((3, TAPS, channels), F32),
            jax.ShapeDtypeStruct((1, channels), F32),
        ),
        in_specs=[whole],
        out_specs=(far,) * 5,
        scratch_shapes=[
            pltpu.VMEM((3, TAPS, channels), F32),
            pltpu.VMEM((1, channels), F32),
            pltpu.SemaphoreType.DMA((STREAMS + 2,)),
        ],
    )(back)
    return (
        gated_out.reshape(channels, LANES),
        feature_grad.reshape(3, channels, LANES),
        long_grad.reshape(channels, LANES),
        jnp.swapaxes(short_grad, 1, 2),
        skip_grad.reshape(channels),
    )


def solution(mesh):
    torus = Mesh(mesh.devices.reshape(*SIDES, mesh.shape["chan"]), (*SEQ, "chan"))
    return jax.shard_map(
        shards,
        mesh=torus,
        in_specs=(
            P(None, "chan", SEQ),
            P("chan", SEQ),
            P("chan", SEQ),
            P(None, "chan", None),
            P("chan"),
        ),
        out_specs=(
            P("chan", SEQ),
            P(None, "chan", SEQ),
            P("chan", SEQ),
            P(None, "chan", None),
            P("chan"),
        ),
        check_vma=False,
    )
```

```python
import jax
import jax.numpy as jnp
from jax import lax
from jax.experimental import pallas as pl
from jax.experimental.pallas import tpu as pltpu
from jax.sharding import Mesh
from jax.sharding import PartitionSpec as P

SEQ = ("x", "y", "c")
SIDES = (4, 2, 2)
ENTRY = ("c", "y", "x")
OWNERS = ("c", "x")
BLOCKS = 16
GROUPS = 8
EACH = 8
LANES = 128
STREAMS = 5
TAPS = 3
SUMS = 3 * TAPS + 1
IN_ROWS = STREAMS * EACH
OUT_ROWS = IN_ROWS + 16
PHASES = 4
STEP = LANES // PHASES

F32 = jnp.float32
BF16 = jnp.bfloat16


def iota(shape, dim):
    return lax.broadcasted_iota(jnp.int32, shape, dim)


def pack_kernel(features, cotangent, long_filter, weights, gain, out, table, taps, gains, sems):
    small = [
        pltpu.make_async_copy(weights, taps, sems.at[0]),
        pltpu.make_async_copy(gain, gains, sems.at[1]),
    ]
    sources = [features.at[i] for i in range(3)] + [cotangent, long_filter]
    large = []
    for i, source in enumerate(sources):
        target = out.at[:, 0, :, pl.ds(i * EACH, EACH), :]
        large.append(pltpu.make_async_copy(source, target, sems.at[2 + i]))
    for copy in small + large:
        copy.start()
    for copy in small:
        copy.wait()
    first = (lax.axis_index("c") * SIDES[0] + lax.axis_index("x")) * EACH
    channels = gains.shape[1]
    shape = (EACH, channels)
    chosen = iota(shape, 1) == iota(shape, 0) + first
    for j in range(SUMS):
        line = gains[...] if j == 3 * TAPS else taps[j // TAPS, j % TAPS : j % TAPS + 1, :]
        line = jnp.broadcast_to(line, shape)
        column = jnp.sum(jnp.where(chosen, line, 0.0), axis=1, keepdims=True)
        table[j] = jnp.broadcast_to(column, (EACH, LANES))
    for i, copy in enumerate(large):
        copy.wait()
        cut = slice(i * EACH, (i + 1) * EACH)
        out[:, 1, :, cut, :] = out[:, 0, :, cut, :]


def after(values, before, count):
    mixed = jnp.where(iota(values.shape, 1) < LANES - count, values, before)
    return pltpu.roll(mixed, count, 1)


def ahead(values, behind, count):
    mixed = jnp.where(iota(values.shape, 1) >= count, values, behind)
    return pltpu.roll(mixed, LANES - count, 1)


def fill_right(line_of, right):
    shape = (STEP, LANES)
    keep = iota(shape, 1) >= iota(shape, 0)
    before = jnp.zeros(shape, F32)
    for k in range(BLOCKS):
        line = jnp.broadcast_to(line_of(k), shape)
        turned = pltpu.roll(line, 0, 1, stride=1, stride_axis=0)
        part = jnp.where(keep, turned, before).astype(BF16)
        right[k * STEP : (k + 1) * STEP, :] = part
        before = turned


def shifted_down(values, count):
    if count == 0:
        return values
    whole, rest = divmod(count, 8)
    parts = [values[n : n + 8] for n in range(0, values.shape[0], 8)]
    zero = jnp.zeros_like(parts[0])
    if rest:
        keep = iota(zero.shape, 0) >= rest
        turned = [pltpu.roll(part, rest, 0) for part in parts]
        parts = [jnp.where(keep, t, b) for t, b in zip(turned, [zero] + turned[:-1])]
    return jnp.concatenate([zero] * whole + parts[: len(parts) - whole], axis=0)


def shifted_up(values, count):
    if count == 0:
        return values
    whole, rest = divmod(count, 8)
    parts = [values[n : n + 8] for n in range(0, values.shape[0], 8)]
    zero = jnp.zeros_like(parts[0])
    if rest:
        keep = iota(zero.shape, 0) < 8 - rest
        turned = [pltpu.roll(part, 8 - rest, 0) for part in parts]
        parts = [jnp.where(keep, t, b) for t, b in zip(turned, turned[1:] + [zero])]
    return jnp.concatenate(parts[whole:] + [zero] * whole, axis=0)


def left_rows(values, shifted):
    turned = [pltpu.roll(values, STEP * q, 1) if q else values for q in range(PHASES)]
    moved = [[shifted(turned[q], kk) for q in range(PHASES)] for kk in range(PHASES)]
    part = iota(values.shape, 1) // STEP
    rows = []
    for p in range(PHASES):
        base = moved[0][-p % PHASES]
        for kk in range(1, PHASES):
            base = jnp.where(part == kk, moved[kk][(kk - p) % PHASES], base)
        tiles = [shifted(base, PHASES * j).astype(BF16) for j in range(BLOCKS // PHASES)]
        rows.append(jnp.concatenate(tiles, axis=1))
    return rows


def joined(parts, shifted):
    total = parts[0]
    for p in range(1, PHASES):
        total = total + after(parts[p], shifted(parts[p], 1), STEP * p)
    return total


def middle_kernel(
    table, received, out, wide, packed, right, kept, mirrored, turned_back, left, product, sums
):
    pad = jnp.zeros((IN_ROWS, LANES), F32)
    wide[0:IN_ROWS, :] = pad
    wide[(BLOCKS + 1) * IN_ROWS : (BLOCKS + 2) * IN_ROWS, :] = pad
    for c in range(SIDES[2]):
        for y in range(SIDES[1]):
            for x in range(SIDES[0]):
                source = (c * SIDES[1] + y) * SIDES[0] + x
                at = ((x * SIDES[1] + y) * SIDES[2] + c + 1) * IN_ROWS
                wide[at : at + IN_ROWS, :] = received[source].astype(F32)
    square = (LANES, LANES)
    mirror = jnp.where(iota(square, 0) + iota(square, 1) == LANES - 1, 1.0, 0.0).astype(BF16)

    def stream(i, c, back=0):
        at = (1 - back) * IN_ROWS + i * EACH + c
        return wide[pl.ds(at, BLOCKS, stride=IN_ROWS), :]

    def put(i, c, values):
        packed[pl.ds(i * EACH + c, BLOCKS, stride=IN_ROWS), :] = values

    def weight(j, c):
        return table[j, c : c + 1, :]

    def rows(c):
        return slice(c * BLOCKS, (c + 1) * BLOCKS)

    PRIMED, MIXED, GATED, HISTORY, LONG = 0, 3, 4, 5, 11
    half = EACH * BLOCKS

    def add(j, c, values):
        at = (j * EACH + c) * 8
        sums[at : at + 8, :] = values[0:8] + values[8:16]

    def prime(c):
        primed = []
        for i in range(3):
            value, before = stream(i, c), stream(i, c, 1)
            running = weight(i * TAPS, c) * value
            for o in range(1, TAPS):
                moved = after(value, before, o)
                kept[HISTORY + 2 * i + o - 1, rows(c), :] = moved
                running = running + weight(i * TAPS + o, c) * moved
            kept[PRIMED + i, rows(c), :] = running
            primed.append(running)
        kept[MIXED, rows(c), :] = (primed[1] * primed[2]).astype(BF16).astype(F32)
        kept[GATED, rows(c), :] = (stream(3, c) * primed[0]).astype(BF16).astype(F32)

    def reflect(ref, start, values):
        ref[start : start + BLOCKS, :] = jnp.dot(
            values.astype(BF16), mirror, preferred_element_type=F32
        )

    def filter_band(c):
        at = IN_ROWS + 4 * EACH + c
        fill_right(lambda k: wide[at + k * IN_ROWS : at + k * IN_ROWS + 1, :], right.at[c, 0])

    def mixed_band(c):
        at = c * BLOCKS
        fill_right(lambda k: kept[MIXED, at + k : at + k + 1, :], right.at[c, 1])

    def turn(c):
        reflect(mirrored, c * BLOCKS, kept[GATED, rows(c), :])

    def mixed_rows(c):
        lines = left_rows(kept[MIXED, rows(c), :], shifted_down)
        left[c, 0 : PHASES * BLOCKS, :] = jnp.concatenate(lines, axis=0)

    def gated_rows(c):
        lines = left_rows(mirrored[rows(c), :], shifted_up)
        left[c, PHASES * BLOCKS :, :] = jnp.concatenate(lines, axis=0)

    def multiply(c):
        band = jnp.concatenate([right[c, 0], right[c, 1]], axis=1)
        product[c] = jnp.dot(left[c], band, preferred_element_type=F32)

    def parts(c, first, column):
        lines = [first + p * BLOCKS for p in range(PHASES)]
        return [product[c, n : n + BLOCKS, column : column + LANES] for n in lines]

    def gather(c):
        gain = weight(3 * TAPS, c)
        conv = joined(parts(c, 0, 0), shifted_down)
        corr = joined(parts(c, PHASES * BLOCKS, 0), shifted_up)
        cross = joined(parts(c, PHASES * BLOCKS, LANES), shifted_up)
        kept[LONG, rows(c), :] = (conv + gain * kept[MIXED, rows(c), :]).astype(BF16).astype(F32)
        turned_back[rows(c), :] = corr + gain * mirrored[rows(c), :]
        turned_back[half + c * BLOCKS : half + (c + 1) * BLOCKS, :] = cross

    def turn_back(c):
        for start in (c * BLOCKS, half + c * BLOCKS):
            reflect(turned_back, start, turned_back[start : start + BLOCKS, :])

    def finish(c):
        cot = stream(3, c)
        primed = [kept[PRIMED + i, rows(c), :] for i in range(3)]
        long_out = kept[LONG, rows(c), :]
        mixed_grad = turned_back[rows(c), :]
        primed_grad = [cot * long_out, mixed_grad * primed[2], mixed_grad * primed[1]]
        put(0, c, primed[0] * long_out)
        put(4, c, turned_back[half + c * BLOCKS : half + (c + 1) * BLOCKS, :])
        for i in range(3):
            behind = shifted_up(primed_grad[i], 1)
            running = weight(i * TAPS, c) * primed_grad[i]
            for o in range(1, TAPS):
                running = running + weight(i * TAPS + o, c) * ahead(primed_grad[i], behind, o)
            put(1 + i, c, running)
            for o in range(TAPS):
                past = kept[HISTORY + 2 * i + o - 1, rows(c), :] if o else stream(i, c)
                add(i * TAPS + o, c, primed_grad[i] * past)
        add(3 * TAPS, c, kept[GATED, rows(c), :] * kept[MIXED, rows(c), :])

    for c in range(EACH):
        prime(c)
    for c in range(EACH):
        turn(c)
    for c in range(EACH):
        filter_band(c)
        mixed_rows(c)
    for c in range(EACH):
        mixed_band(c)
        gated_rows(c)
    for c in range(EACH):
        multiply(c)
    for c in range(EACH):
        gather(c)
    for c in range(EACH):
        turn_back(c)
    for c in range(EACH):
        finish(c)
    lines = []
    for j in range(SUMS):
        line = sums[pl.ds(j * EACH * 8, EACH, stride=8), :]
        for n in range(1, 8):
            line = line + sums[pl.ds(j * EACH * 8 + n, EACH, stride=8), :]
        lines.append(line)
    stacked = jnp.concatenate(lines, axis=0)
    totals = jnp.sum(stacked, axis=1, keepdims=True)
    upper = totals.astype(BF16).astype(F32)
    shape = (SUMS, EACH, LANES)
    upper = jnp.broadcast_to(upper, stacked.shape).reshape(shape)
    totals = jnp.broadcast_to(totals, stacked.shape).reshape(shape)
    channels = GROUPS * EACH
    lane = iota(shape, 2)
    first = (lax.axis_index("c") * SIDES[0] + lax.axis_index("x")) * EACH
    both = jnp.where(lane < channels, upper, totals - upper)
    mine = lane % channels == iota(shape, 1) + first
    lines = jnp.sum(jnp.where(mine, both, 0.0), axis=1)
    rest = jnp.zeros((OUT_ROWS - IN_ROWS - SUMS, LANES), F32)
    lines = jnp.concatenate([lines, rest], axis=0).astype(BF16)
    side = lax.axis_index("y")
    for c in range(SIDES[2]):
        for x in range(SIDES[0]):
            block = (x * SIDES[1] + side) * SIDES[2] + c
            at = pl.multiple_of(block * IN_ROWS, 8)
            out[c * SIDES[0] + x, 0:IN_ROWS, :] = packed[pl.ds(at, IN_ROWS), :].astype(BF16)
    for n in range(GROUPS):
        out[n, IN_ROWS:OUT_ROWS, :] = lines


def unpack_kernel(
    received, gated_out, feature_grad, long_grad, short_grad, skip_grad, taps, gains, sems
):
    targets = [gated_out] + [feature_grad.at[i] for i in range(3)] + [long_grad]
    copies = []
    for i, target in enumerate(targets):
        source = received.at[:, pl.ds(i * EACH, EACH), :]
        copies.append(pltpu.make_async_copy(source, target, sems.at[i]))
        copies[-1].start()
    lines = jnp.sum(received[:, IN_ROWS:OUT_ROWS, :].astype(F32), axis=0)
    lines = lines + pltpu.roll(lines, LANES // 2, 1)
    channels = gains.shape[1]
    for i in range(3):
        taps[i] = lines[i * TAPS : (i + 1) * TAPS, 0:channels]
    gains[...] = lines[3 * TAPS : SUMS, 0:channels]
    last = [
        pltpu.make_async_copy(taps, short_grad, sems.at[STREAMS]),
        pltpu.make_async_copy(gains, skip_grad, sems.at[STREAMS + 1]),
    ]
    for copy in last:
        copy.start()
    for copy in copies + last:
        copy.wait()


def grant(mebibytes):
    return pltpu.CompilerParams(vmem_limit_bytes=mebibytes << 20)


def stay(array):
    return pltpu.with_memory_space_constraint(array, pltpu.HBM)


def shards(features, cotangent, long_filter, short_filters, skip_gain):
    channels = features.shape[1]
    whole = pl.BlockSpec(memory_space=pltpu.VMEM)
    far = pl.BlockSpec(memory_space=pltpu.HBM)
    cut = (SIDES[2], SIDES[0], EACH, LANES)
    parts, table = pl.pallas_call(
        pack_kernel,
        name="pack",
        compiler_params=grant(4),
        out_shape=(
            jax.ShapeDtypeStruct((*SIDES[::-1], IN_ROWS, LANES), BF16),
            jax.ShapeDtypeStruct((SUMS, EACH, LANES), F32),
        ),
        in_specs=[far] * 5,
        out_specs=(whole, whole),
        scratch_shapes=[
            pltpu.VMEM((3, TAPS, channels), F32),
            pltpu.VMEM((1, channels), F32),
            pltpu.SemaphoreType.DMA((2 + STREAMS,)),
        ],
    )(
        stay(features.reshape(3, *cut)),
        stay(cotangent.reshape(cut)),
        stay(long_filter.reshape(cut)),
        stay(jnp.swapaxes(short_filters, 1, 2)),
        stay(skip_gain.reshape(1, channels)),
    )
    columns = lax.all_to_all(
        parts.reshape(BLOCKS, IN_ROWS, LANES), ENTRY, split_axis=0, concat_axis=0, tiled=True
    )
    results = pl.pallas_call(
        middle_kernel,
        name="middle",
        compiler_params=grant(12),
        out_shape=jax.ShapeDtypeStruct((GROUPS, OUT_ROWS, LANES), BF16),
        in_specs=[whole, whole],
        out_specs=whole,
        scratch_shapes=[
            pltpu.VMEM(((BLOCKS + 2) * IN_ROWS, LANES), F32),
            pltpu.VMEM((BLOCKS * IN_ROWS, LANES), F32),
            pltpu.VMEM((EACH, 2, BLOCKS * STEP, LANES), BF16),
            pltpu.VMEM((12, EACH * BLOCKS, LANES), F32),
            pltpu.VMEM((EACH * BLOCKS, LANES), F32),
            pltpu.VMEM((2 * EACH * BLOCKS, LANES), F32),
            pltpu.VMEM((EACH, 2 * PHASES * BLOCKS, BLOCKS * STEP), BF16),
            pltpu.VMEM((EACH, 2 * PHASES * BLOCKS, 2 * LANES), F32),
            pltpu.VMEM((SUMS * EACH * 8, LANES), F32),
        ],
    )(table, columns)
    back = lax.all_to_all(results, OWNERS, split_axis=0, concat_axis=0, tiled=True)
    block = (GROUPS, EACH, LANES)
    gated_out, feature_grad, long_grad, short_grad, skip_grad = pl.pallas_call(
        unpack_kernel,
        name="unpack",
        compiler_params=grant(4),
        out_shape=(
            jax.ShapeDtypeStruct(block, BF16),
            jax.ShapeDtypeStruct((3, *block), BF16),
            jax.ShapeDtypeStruct(block, BF16),
            jax.ShapeDtypeStruct((3, TAPS, channels), F32),
            jax.ShapeDtypeStruct((1, channels), F32),
        ),
        in_specs=[whole],
        out_specs=(far,) * 5,
        scratch_shapes=[
            pltpu.VMEM((3, TAPS, channels), F32),
            pltpu.VMEM((1, channels), F32),
            pltpu.SemaphoreType.DMA((STREAMS + 2,)),
        ],
    )(back)
    return (
        gated_out.reshape(channels, LANES),
        feature_grad.reshape(3, channels, LANES),
        long_grad.reshape(channels, LANES),
        jnp.swapaxes(short_grad, 1, 2),
        skip_grad.reshape(channels),
    )


def solution(mesh):
    torus = Mesh(mesh.devices.reshape(*SIDES, mesh.shape["chan"]), (*SEQ, "chan"))
    return jax.shard_map(
        shards,
        mesh=torus,
        in_specs=(
            P(None, "chan", SEQ),
            P("chan", SEQ),
            P("chan", SEQ),
            P(None, "chan", None),
            P("chan"),
        ),
        out_specs=(
            P("chan", SEQ),
            P(None, "chan", SEQ),
            P("chan", SEQ),
            P(None, "chan", None),
            P("chan"),
        ),
        check_vma=False,
    )
```

```python
import jax
import jax.numpy as jnp
from jax import lax
from jax.experimental import pallas as pl
from jax.experimental.pallas import tpu as pltpu
from jax.sharding import Mesh
from jax.sharding import PartitionSpec as P

SEQ = ("x", "y", "c")
SIDES = (4, 2, 2)
ENTRY = ("c", "y", "x")
OWNERS = ("c", "x")
BLOCKS = 16
GROUPS = 8
EACH = 8
LANES = 128
STREAMS = 5
TAPS = 3
SUMS = 3 * TAPS + 1
IN_ROWS = STREAMS * EACH
OUT_ROWS = IN_ROWS + 16
PHASES = 4
STEP = LANES // PHASES

F32 = jnp.float32
BF16 = jnp.bfloat16


def iota(shape, dim):
    return lax.broadcasted_iota(jnp.int32, shape, dim)


def pack_kernel(features, cotangent, long_filter, weights, gain, out, table, taps, gains, sems):
    small = [
        pltpu.make_async_copy(weights, taps, sems.at[0]),
        pltpu.make_async_copy(gain, gains, sems.at[1]),
    ]
    sources = [features.at[i] for i in range(3)] + [cotangent, long_filter]
    large = []
    for i, source in enumerate(sources):
        target = out.at[:, 0, :, pl.ds(i * EACH, EACH), :]
        large.append(pltpu.make_async_copy(source, target, sems.at[2 + i]))
    for copy in small + large:
        copy.start()
    for copy in small:
        copy.wait()
    first = (lax.axis_index("c") * SIDES[0] + lax.axis_index("x")) * EACH
    channels = gains.shape[1]
    shape = (EACH, channels)
    chosen = iota(shape, 1) == iota(shape, 0) + first
    for j in range(SUMS):
        line = gains[...] if j == 3 * TAPS else taps[j // TAPS, j % TAPS : j % TAPS + 1, :]
        line = jnp.broadcast_to(line, shape)
        column = jnp.sum(jnp.where(chosen, line, 0.0), axis=1, keepdims=True)
        table[j] = jnp.broadcast_to(column, (EACH, LANES))
    for copy in large:
        copy.wait()
    out[:, 1] = out[:, 0]


def after(values, before, count):
    mixed = jnp.where(iota(values.shape, 1) < LANES - count, values, before)
    return pltpu.roll(mixed, count, 1)


def ahead(values, behind, count):
    mixed = jnp.where(iota(values.shape, 1) >= count, values, behind)
    return pltpu.roll(mixed, LANES - count, 1)


def fill_right(line_of, right):
    shape = (STEP, LANES)
    keep = iota(shape, 1) >= iota(shape, 0)
    before = jnp.zeros(shape, F32)
    for k in range(BLOCKS):
        line = jnp.broadcast_to(line_of(k), shape)
        turned = pltpu.roll(line, 0, 1, stride=1, stride_axis=0)
        part = jnp.where(keep, turned, before).astype(BF16)
        right[k * STEP : (k + 1) * STEP, :] = part
        before = turned


def shifted_down(values, count):
    if count == 0:
        return values
    whole, rest = divmod(count, 8)
    parts = [values[n : n + 8] for n in range(0, values.shape[0], 8)]
    zero = jnp.zeros_like(parts[0])
    if rest:
        keep = iota(zero.shape, 0) >= rest
        turned = [pltpu.roll(part, rest, 0) for part in parts]
        parts = [jnp.where(keep, t, b) for t, b in zip(turned, [zero] + turned[:-1])]
    return jnp.concatenate([zero] * whole + parts[: len(parts) - whole], axis=0)


def shifted_up(values, count):
    if count == 0:
        return values
    whole, rest = divmod(count, 8)
    parts = [values[n : n + 8] for n in range(0, values.shape[0], 8)]
    zero = jnp.zeros_like(parts[0])
    if rest:
        keep = iota(zero.shape, 0) < 8 - rest
        turned = [pltpu.roll(part, 8 - rest, 0) for part in parts]
        parts = [jnp.where(keep, t, b) for t, b in zip(turned, turned[1:] + [zero])]
    return jnp.concatenate(parts[whole:] + [zero] * whole, axis=0)


def left_rows(values, shifted):
    turned = [pltpu.roll(values, STEP * q, 1) if q else values for q in range(PHASES)]
    moved = [[shifted(turned[q], kk) for q in range(PHASES)] for kk in range(PHASES)]
    part = iota(values.shape, 1) // STEP
    rows = []
    for p in range(PHASES):
        base = moved[0][-p % PHASES]
        for kk in range(1, PHASES):
            base = jnp.where(part == kk, moved[kk][(kk - p) % PHASES], base)
        tiles = [shifted(base, PHASES * j).astype(BF16) for j in range(BLOCKS // PHASES)]
        rows.append(jnp.concatenate(tiles, axis=1))
    return rows


def joined(parts, shifted):
    total = parts[0]
    for p in range(1, PHASES):
        total = total + after(parts[p], shifted(parts[p], 1), STEP * p)
    return total


def middle_kernel(
    table, received, out, wide, packed, right, kept, mirrored, turned_back, left, product, sums
):
    pad = jnp.zeros((IN_ROWS, LANES), F32)
    wide[0:IN_ROWS, :] = pad
    wide[(BLOCKS + 1) * IN_ROWS : (BLOCKS + 2) * IN_ROWS, :] = pad
    for c in range(SIDES[2]):
        for y in range(SIDES[1]):
            for x in range(SIDES[0]):
                source = (c * SIDES[1] + y) * SIDES[0] + x
                at = ((x * SIDES[1] + y) * SIDES[2] + c + 1) * IN_ROWS
                wide[at : at + IN_ROWS, :] = received[source].astype(F32)
    square = (LANES, LANES)
    mirror = jnp.where(iota(square, 0) + iota(square, 1) == LANES - 1, 1.0, 0.0).astype(BF16)

    def stream(i, c, back=0):
        at = (1 - back) * IN_ROWS + i * EACH + c
        return wide[pl.ds(at, BLOCKS, stride=IN_ROWS), :]

    def put(i, c, values):
        packed[pl.ds(i * EACH + c, BLOCKS, stride=IN_ROWS), :] = values

    def weight(j, c):
        return table[j, c : c + 1, :]

    def rows(c):
        return slice(c * BLOCKS, (c + 1) * BLOCKS)

    PRIMED, MIXED, GATED, HISTORY, LONG = 0, 3, 4, 5, 11
    half = EACH * BLOCKS

    def add(j, c, values):
        at = (j * EACH + c) * 8
        sums[at : at + 8, :] = values[0:8] + values[8:16]

    def prime(c):
        primed = []
        for i in range(3):
            value, before = stream(i, c), stream(i, c, 1)
            running = weight(i * TAPS, c) * value
            for o in range(1, TAPS):
                moved = after(value, before, o)
                kept[HISTORY + 2 * i + o - 1, rows(c), :] = moved
                running = running + weight(i * TAPS + o, c) * moved
            kept[PRIMED + i, rows(c), :] = running
            primed.append(running)
        kept[MIXED, rows(c), :] = (primed[1] * primed[2]).astype(BF16).astype(F32)
        kept[GATED, rows(c), :] = (stream(3, c) * primed[0]).astype(BF16).astype(F32)

    def reflect(ref, start, values):
        ref[start : start + BLOCKS, :] = jnp.dot(
            values.astype(BF16), mirror, preferred_element_type=F32
        )

    def filter_band(c):
        at = IN_ROWS + 4 * EACH + c
        fill_right(lambda k: wide[at + k * IN_ROWS : at + k * IN_ROWS + 1, :], right.at[c, 0])

    def mixed_band(c):
        at = c * BLOCKS
        fill_right(lambda k: kept[MIXED, at + k : at + k + 1, :], right.at[c, 1])

    def turn(c):
        reflect(mirrored, c * BLOCKS, kept[GATED, rows(c), :])

    def mixed_rows(c):
        lines = left_rows(kept[MIXED, rows(c), :], shifted_down)
        left[c, 0 : PHASES * BLOCKS, :] = jnp.concatenate(lines, axis=0)

    def gated_rows(c):
        lines = left_rows(mirrored[rows(c), :], shifted_up)
        left[c, PHASES * BLOCKS :, :] = jnp.concatenate(lines, axis=0)

    def multiply(c):
        band = jnp.concatenate([right[c, 0], right[c, 1]], axis=1)
        product[c] = jnp.dot(left[c], band, preferred_element_type=F32)

    def parts(c, first, column):
        lines = [first + p * BLOCKS for p in range(PHASES)]
        return [product[c, n : n + BLOCKS, column : column + LANES] for n in lines]

    def gather(c):
        gain = weight(3 * TAPS, c)
        conv = joined(parts(c, 0, 0), shifted_down)
        corr = joined(parts(c, PHASES * BLOCKS, 0), shifted_up)
        cross = joined(parts(c, PHASES * BLOCKS, LANES), shifted_up)
        kept[LONG, rows(c), :] = (conv + gain * kept[MIXED, rows(c), :]).astype(BF16).astype(F32)
        turned_back[rows(c), :] = corr + gain * mirrored[rows(c), :]
        turned_back[half + c * BLOCKS : half + (c + 1) * BLOCKS, :] = cross

    def turn_back(c):
        for start in (c * BLOCKS, half + c * BLOCKS):
            reflect(turned_back, start, turned_back[start : start + BLOCKS, :])

    def finish(c):
        cot = stream(3, c)
        primed = [kept[PRIMED + i, rows(c), :] for i in range(3)]
        long_out = kept[LONG, rows(c), :]
        mixed_grad = turned_back[rows(c), :]
        primed_grad = [cot * long_out, mixed_grad * primed[2], mixed_grad * primed[1]]
        put(0, c, primed[0] * long_out)
        put(4, c, turned_back[half + c * BLOCKS : half + (c + 1) * BLOCKS, :])
        for i in range(3):
            behind = shifted_up(primed_grad[i], 1)
            running = weight(i * TAPS, c) * primed_grad[i]
            for o in range(1, TAPS):
                running = running + weight(i * TAPS + o, c) * ahead(primed_grad[i], behind, o)
            put(1 + i, c, running)
            for o in range(TAPS):
                past = kept[HISTORY + 2 * i + o - 1, rows(c), :] if o else stream(i, c)
                add(i * TAPS + o, c, primed_grad[i] * past)
        add(3 * TAPS, c, kept[GATED, rows(c), :] * kept[MIXED, rows(c), :])

    for c in range(EACH + 4):
        if 0 <= c < EACH + 0:
            prime(c - 0)
        if 4 <= c < EACH + 4:
            turn(c - 4)
    for c in range(EACH):
        filter_band(c)
        mixed_rows(c)
    for c in range(EACH):
        mixed_band(c)
        gated_rows(c)
    for c in range(EACH):
        multiply(c)
    for c in range(EACH):
        gather(c)
    for c in range(EACH + 4):
        if 0 <= c < EACH + 0:
            turn_back(c - 0)
        if 4 <= c < EACH + 4:
            finish(c - 4)
    lines = []
    for j in range(SUMS):
        line = sums[pl.ds(j * EACH * 8, EACH, stride=8), :]
        for n in range(1, 8):
            line = line + sums[pl.ds(j * EACH * 8 + n, EACH, stride=8), :]
        lines.append(line)
    stacked = jnp.concatenate(lines, axis=0)
    totals = jnp.sum(stacked, axis=1, keepdims=True)
    upper = totals.astype(BF16).astype(F32)
    shape = (SUMS, EACH, LANES)
    upper = jnp.broadcast_to(upper, stacked.shape).reshape(shape)
    totals = jnp.broadcast_to(totals, stacked.shape).reshape(shape)
    channels = GROUPS * EACH
    lane = iota(shape, 2)
    first = (lax.axis_index("c") * SIDES[0] + lax.axis_index("x")) * EACH
    both = jnp.where(lane < channels, upper, totals - upper)
    mine = lane % channels == iota(shape, 1) + first
    lines = jnp.sum(jnp.where(mine, both, 0.0), axis=1)
    rest = jnp.zeros((OUT_ROWS - IN_ROWS - SUMS, LANES), F32)
    lines = jnp.concatenate([lines, rest], axis=0).astype(BF16)
    side = lax.axis_index("y")
    for c in range(SIDES[2]):
        for x in range(SIDES[0]):
            block = (x * SIDES[1] + side) * SIDES[2] + c
            at = pl.multiple_of(block * IN_ROWS, 8)
            out[c * SIDES[0] + x, 0:IN_ROWS, :] = packed[pl.ds(at, IN_ROWS), :].astype(BF16)
    for n in range(GROUPS):
        out[n, IN_ROWS:OUT_ROWS, :] = lines


def unpack_kernel(
    received, gated_out, feature_grad, long_grad, short_grad, skip_grad, taps, gains, sems
):
    targets = [gated_out] + [feature_grad.at[i] for i in range(3)] + [long_grad]
    copies = []
    for i, target in enumerate(targets):
        source = received.at[:, pl.ds(i * EACH, EACH), :]
        copies.append(pltpu.make_async_copy(source, target, sems.at[i]))
        copies[-1].start()
    lines = jnp.sum(received[:, IN_ROWS:OUT_ROWS, :].astype(F32), axis=0)
    lines = lines + pltpu.roll(lines, LANES // 2, 1)
    channels = gains.shape[1]
    for i in range(3):
        taps[i] = lines[i * TAPS : (i + 1) * TAPS, 0:channels]
    gains[...] = lines[3 * TAPS : SUMS, 0:channels]
    last = [
        pltpu.make_async_copy(taps, short_grad, sems.at[STREAMS]),
        pltpu.make_async_copy(gains, skip_grad, sems.at[STREAMS + 1]),
    ]
    for copy in last:
        copy.start()
    for copy in copies + last:
        copy.wait()


def grant(mebibytes):
    return pltpu.CompilerParams(vmem_limit_bytes=mebibytes << 20)


def stay(array):
    return pltpu.with_memory_space_constraint(array, pltpu.HBM)


def shards(features, cotangent, long_filter, short_filters, skip_gain):
    channels = features.shape[1]
    whole = pl.BlockSpec(memory_space=pltpu.VMEM)
    far = pl.BlockSpec(memory_space=pltpu.HBM)
    cut = (SIDES[2], SIDES[0], EACH, LANES)
    parts, table = pl.pallas_call(
        pack_kernel,
        name="pack",
        compiler_params=grant(4),
        out_shape=(
            jax.ShapeDtypeStruct((*SIDES[::-1], IN_ROWS, LANES), BF16),
            jax.ShapeDtypeStruct((SUMS, EACH, LANES), F32),
        ),
        in_specs=[far] * 5,
        out_specs=(whole, whole),
        scratch_shapes=[
            pltpu.VMEM((3, TAPS, channels), F32),
            pltpu.VMEM((1, channels), F32),
            pltpu.SemaphoreType.DMA((2 + STREAMS,)),
        ],
    )(
        stay(features.reshape(3, *cut)),
        stay(cotangent.reshape(cut)),
        stay(long_filter.reshape(cut)),
        stay(jnp.swapaxes(short_filters, 1, 2)),
        stay(skip_gain.reshape(1, channels)),
    )
    columns = lax.all_to_all(
        parts.reshape(BLOCKS, IN_ROWS, LANES), ENTRY, split_axis=0, concat_axis=0, tiled=True
    )
    results = pl.pallas_call(
        middle_kernel,
        name="middle",
        compiler_params=grant(12),
        out_shape=jax.ShapeDtypeStruct((GROUPS, OUT_ROWS, LANES), BF16),
        in_specs=[whole, whole],
        out_specs=whole,
        scratch_shapes=[
            pltpu.VMEM(((BLOCKS + 2) * IN_ROWS, LANES), F32),
            pltpu.VMEM((BLOCKS * IN_ROWS, LANES), F32),
            pltpu.VMEM((EACH, 2, BLOCKS * STEP, LANES), BF16),
            pltpu.VMEM((12, EACH * BLOCKS, LANES), F32),
            pltpu.VMEM((EACH * BLOCKS, LANES), F32),
            pltpu.VMEM((2 * EACH * BLOCKS, LANES), F32),
            pltpu.VMEM((EACH, 2 * PHASES * BLOCKS, BLOCKS * STEP), BF16),
            pltpu.VMEM((EACH, 2 * PHASES * BLOCKS, 2 * LANES), F32),
            pltpu.VMEM((SUMS * EACH * 8, LANES), F32),
        ],
    )(table, columns)
    back = lax.all_to_all(results, OWNERS, split_axis=0, concat_axis=0, tiled=True)
    block = (GROUPS, EACH, LANES)
    gated_out, feature_grad, long_grad, short_grad, skip_grad = pl.pallas_call(
        unpack_kernel,
        name="unpack",
        compiler_params=grant(4),
        out_shape=(
            jax.ShapeDtypeStruct(block, BF16),
            jax.ShapeDtypeStruct((3, *block), BF16),
            jax.ShapeDtypeStruct(block, BF16),
            jax.ShapeDtypeStruct((3, TAPS, channels), F32),
            jax.ShapeDtypeStruct((1, channels), F32),
        ),
        in_specs=[whole],
        out_specs=(far,) * 5,
        scratch_shapes=[
            pltpu.VMEM((3, TAPS, channels), F32),
            pltpu.VMEM((1, channels), F32),
            pltpu.SemaphoreType.DMA((STREAMS + 2,)),
        ],
    )(back)
    return (
        gated_out.reshape(channels, LANES),
        feature_grad.reshape(3, channels, LANES),
        long_grad.reshape(channels, LANES),
        jnp.swapaxes(short_grad, 1, 2),
        skip_grad.reshape(channels),
    )


def solution(mesh):
    torus = Mesh(mesh.devices.reshape(*SIDES, mesh.shape["chan"]), (*SEQ, "chan"))
    return jax.shard_map(
        shards,
        mesh=torus,
        in_specs=(
            P(None, "chan", SEQ),
            P("chan", SEQ),
            P("chan", SEQ),
            P(None, "chan", None),
            P("chan"),
        ),
        out_specs=(
            P("chan", SEQ),
            P(None, "chan", SEQ),
            P("chan", SEQ),
            P(None, "chan", None),
            P("chan"),
        ),
        check_vma=False,
    )
```
